128 devices in a mesh: gx: 2 (over core), gy: 4 (over x), gz: 16 (over z, y).
Axes of the slice: x: 4, y: 4, z: 4, core: 2. Of those that a mesh axis runs over, the one named last changes fastest.
Arguments:
- permanent_field: float32 [12, 24, 96, 3], P('gx', 'gy', 'gz'), may hold values from -6 to 6
- polar: float32 [12, 24, 96], P('gx', 'gy', 'gz'), may hold values from 0.4 to 1.4
- jitter: float32 [12, 24, 96, 3], P('gx', 'gy', 'gz'), may hold values from -0.2 to 0.2
- neighbors: int32 [12, 24, 96, 56], P('gx', 'gy', 'gz'), may hold values from -1 to 987, as said below
Outputs:
- dipoles: float32 [12, 24, 96, 3], P('gx', 'gy', 'gz')
- residual: float32 [12, 24, 96, 3], P('gx', 'gy', 'gz')
- step_lengths: float32 [8], replicated
The draws below stay inside these ranges and needn't reach their ends.
Inputs may be any that keep to these rules, and one draw needn't show every extreme that they name: `neighbors`: each entry is -1 or the flat index of a neighbour in the device's block extended by two sites on every side, with an offset d of squared length 1 to 5 (each component -2 to 2), each offset at most once in a row; the -1 entries come after all others; if site j stands in site i's row with offset d then i stands in j's row with offset -d, the box being periodic.
All inputs are finite; a program needn't handle non-finite values.
Results may differ from the reference program's by a relative error of at most 0.0003.
Values sent between devices are 32-bit elements.
A program may use at most 64 MiB of HBM per device.

```python
import math
import jax
import jax.numpy as jnp
from jax import lax

EDGE = 6
ITERS = 8
LX = 12
LY = 24
LZ = 96


def stencil_offsets():
    listed = []
    for shift_x in range(-2, 3):
        for shift_y in range(-2, 3):
            for shift_z in range(-2, 3):
                length = shift_x * shift_x + shift_y * shift_y + shift_z * shift_z
                if 1 <= length <= 5:
                    listed.append((shift_x, shift_y, shift_z))
    return listed


def draw_neighbors(key, part):
    listed = stencil_offsets()
    forward = [offset for offset in listed if offset > (0, 0, 0)]
    coin_bits = jax.random.randint(key, (LX, LY, LZ, len(forward)), 0, 4)
    bonded = (coin_bits < 3).astype(jnp.int32)
    padded_edge = EDGE + 4
    home_x = lax.broadcasted_iota(jnp.int32, (LX, LY, LZ), 0) % EDGE
    home_y = lax.broadcasted_iota(jnp.int32, (LX, LY, LZ), 1) % EDGE
    home_z = lax.broadcasted_iota(jnp.int32, (LX, LY, LZ), 2) % EDGE
    bond_flags = []
    places = []
    for offset in listed:
        if offset > (0, 0, 0):
            bond_flags.append(bonded[..., forward.index(offset)])
        else:
            mirror = (-offset[0], -offset[1], -offset[2])
            bond_flags.append(jnp.roll(bonded[..., forward.index(mirror)], mirror, axis=(0, 1, 2)))
        places.append(((home_x + 2 + offset[0]) * padded_edge + home_y + 2 + offset[1]) * padded_edge + home_z + 2 + offset[2])
    flagged = jnp.stack(bond_flags, axis=-1)
    located = jnp.stack(places, axis=-1)
    ranking = (1 - flagged) * 64 + lax.broadcasted_iota(jnp.int32, flagged.shape, 3)
    ordering = jnp.argsort(ranking, axis=-1, stable=True)
    flagged = jnp.take_along_axis(flagged, ordering, axis=-1)
    located = jnp.take_along_axis(located, ordering, axis=-1)
    return jnp.where(flagged == 1, located, -1).astype(jnp.int32)


def block_levels(own_key, dims, cuts, smallest, high):
    def one(dim, shards_of):
        steps = jax.random.uniform(jax.random.fold_in(jax.random.fold_in(own_key, 6), dim), (shards_of,), jnp.float32, smallest / len(cuts), high / len(cuts))
        return jnp.repeat(jnp.exp(steps), dims[dim] // shards_of).reshape((-1,) + (1,) * (len(dims) - dim - 1))

    factor_of = one(*cuts[0])
    for cut in cuts[1:]:
        factor_of = factor_of * one(*cut)
    return factor_of


def gaussian(rng, shape, width, most, pieces=(), kind=jnp.bfloat16):
    factor_of = block_levels(rng, shape, pieces, -0.22, 0.18) if pieces else 1.0
    result = jax.random.normal(rng, shape, jnp.float32) * width * factor_of
    return jnp.minimum(jnp.maximum(result, -most), most).astype(kind)


def setup_inputs(seed: int = 0) -> dict:
    key_of = jax.random.split(jax.random.key(seed), 5)
    return {
        "permanent_field": gaussian(key_of[0], (LX, LY, LZ, 3), 1.0, 6.0, ((0, 2), (1, 4), (2, 16)), jnp.float32),
        "polar": jnp.clip(jnp.exp(math.log(1.4) - 1.2527629 * jax.random.uniform(key_of[1], (LX, LY, LZ), jnp.float32) ** block_levels(key_of[1], (LX, LY, LZ), ((0, 2), (1, 4), (2, 16)), -0.2, 0.2)), 0.4, 1.4),
        "jitter": jnp.clip(jax.random.uniform(key_of[2], (LX, LY, LZ, 3), jnp.float32, -0.2, 0.2) * block_levels(key_of[2], (LX, LY, LZ, 3), ((0, 2), (1, 4), (2, 16)), -0.4, 0.0), -0.2, 0.2),
        "neighbors": draw_neighbors(jax.random.fold_in(key_of[4], 71), 0),
    }


thole_damping = 0.39
site_spacing = 3.5

def geometry(offsets, jit_self, jit_other, pol_self, pol_other, present):
    separation = (offsets + jit_other - jit_self) * site_spacing
    separation = jnp.where(present[..., None], separation, site_spacing)
    dist_sq = lax.optimization_barrier(jnp.sum(separation * separation, axis=-1))
    distance = jnp.sqrt(dist_sq)
    dist_cube = dist_sq * distance
    damping = thole_damping * dist_cube / jnp.sqrt(pol_self * pol_other)
    falloff = jnp.exp(-damping)
    lam_three = 1.0 - falloff
    lam_five = 1.0 - (1.0 + damping) * falloff
    isotropic = jnp.where(present, lam_three / dist_cube, 0.0)
    radial = jnp.where(present, 3.0 * lam_five / (dist_cube * dist_sq), 0.0)
    return (separation, isotropic, radial)

def couple(separation, isotropic, radial, values):
    projection = lax.optimization_barrier(jnp.sum(separation * values, axis=-1, keepdims=True))
    return lax.optimization_barrier(jnp.sum(radial[..., None] * projection * separation - isotropic[..., None] * values, axis=-2))

def reference(permanent_field, polar, jitter, neighbors):
    padded_edge = EDGE + 4
    flat_jit = jitter.reshape(-1, 3)
    flat_pol = polar.reshape(-1)

    def slab_geometry(inputs):
        row, links, jit_row, pol_row = inputs
        present = links >= 0
        clipped = jnp.where(present, links, 0)
        plane_a = clipped // (padded_edge * padded_edge)
        plane_b = clipped // padded_edge % padded_edge
        plane_c = clipped % padded_edge
        grid_y = lax.broadcasted_iota(jnp.int32, (LY, LZ, 1), 0)
        grid_z = lax.broadcasted_iota(jnp.int32, (LY, LZ, 1), 1)
        shift_x = plane_a - 2 - row % EDGE
        shift_y = plane_b - 2 - grid_y % EDGE
        shift_z = plane_c - 2 - grid_z % EDGE
        other_x = (row + shift_x) % LX
        other_y = (grid_y + shift_y) % LY
        other_z = (grid_z + shift_z) % LZ
        other = ((other_x * LY + other_y) * LZ + other_z).astype(jnp.int32)
        offsets = jnp.stack([shift_x, shift_y, shift_z], axis=-1).astype(jnp.float32)
        separation, isotropic, radial = geometry(offsets, jit_row[:, :, None, :], flat_jit[other], pol_row[:, :, None], flat_pol[other], present)
        return (separation, isotropic, radial, other)
    rows = jnp.arange(LX, dtype=jnp.int32)
    separations, isotropics, radials, others = lax.map(slab_geometry, (rows, neighbors, jitter, polar))

    def operate(vector):
        flat_vec = vector.reshape(-1, 3)

        def slab(inputs):
            separation, isotropic, radial, other = inputs
            return couple(separation, isotropic, radial, flat_vec[other])
        coupled = lax.map(slab, (separations, isotropics, radials, others))
        return vector / polar[..., None] - coupled
    weights = polar[..., None]
    dipoles = weights * permanent_field
    residual = permanent_field - operate(dipoles)
    scaled = weights * residual
    direction = scaled
    gamma_now = jnp.sum(residual * scaled)
    lengths = []
    for number in range(ITERS):
        image = operate(direction)
        step_len = gamma_now / jnp.sum(direction * image)
        dipoles = dipoles + step_len * direction
        residual = residual - step_len * image
        scaled = weights * residual
        gamma_next = jnp.sum(residual * scaled)
        direction = scaled + gamma_next / gamma_now * direction
        gamma_now = gamma_next
        lengths.append(step_len)
    return (dipoles, residual, jnp.stack(lengths))
```

```python
import functools

import jax
import jax.numpy as jnp
from jax import lax
from jax.experimental import pallas as pl
from jax.experimental.pallas import tpu as pltpu
from jax.sharding import PartitionSpec as P

ITERS = 8
BLOCKS = (2, 3, 3)
MESH = pl.DeviceIdType.MESH
thole_damping = 0.39
site_spacing = 3.5
ROWS, LANES = 8, 128
EDGE = 6
WIDE = 3 * EDGE
ORIGIN = 2 * WIDE + 2
OWN = EDGE * WIDE + EDGE - ORIGIN
f32 = jnp.float32

STENCIL = [
    (a, b, c)
    for a in range(-2, 3)
    for b in range(-2, 3)
    for c in range(-2, 3)
    if 1 <= a * a + b * b + c * c <= 5
]
SHIFTS = sorted({(b, c) for a, b, c in STENCIL})
SPAN = [[d[0] for d in STENCIL if d[1:] == s] for s in SHIFTS]
FIRST = [sum(len(v) for v in SPAN[:i]) for i in range(len(SHIFTS))]
HOME = SHIFTS.index((0, 0))
FORWARD = [d for d in STENCIL if d > (0, 0, 0)]


def flag_places():
    room = {0: 9, 1: 10, 2: 10}
    used = {0: 0, 1: 0, 2: 0}
    places = {}
    for d in FORWARD:
        c = d[0] if used[d[0]] < room[d[0]] else 2
        if d[0] != 2 and used[d[0]] >= room[d[0]]:
            c = 2
        places[d] = (c, used[c])
        used[c] += 1
    assert used[2] <= room[2]
    return places


FLAGS = flag_places()
FLAG_TILES = 9
TILES = 3 + FLAG_TILES


def roll(value, shift):
    shift = shift % LANES
    return value if shift == 0 else pltpu.roll(value, shift, axis=1)


def kernel(
    sizes,
    field_ref, pol_ref, jit_ref, nb_ref, x_out, r_out, len_out,
    ext, sh, geo, words, sgeo, sword, polo, coef, chain, state,
    send0, recv0, send1, recv1, dot_src, dot_dst,
    halo_send, halo_recv, dot_send, dot_recv,
):
    nx, ny, nz = sizes
    count = nx * ny * nz
    gx, gy, gz = lax.axis_index("gx"), lax.axis_index("gy"), lax.axis_index("gz")
    rank = (gx * ny + gy) * nz + gz

    def at(ox, oy, oz):
        return (lax.rem(gx + ox + nx, nx), lax.rem(gy + oy + ny, ny), lax.rem(gz + oz + nz, nz))

    others = [
        (a, b, c) for a in range(nx) for b in range(ny) for c in range(nz) if (a, b, c) != (0, 0, 0)
    ]
    others.sort(key=lambda o: -(min(o[0], nx - o[0]) + 2 * min(o[1], ny - o[1]) + 2 * min(o[2], nz - o[2])))

    barrier = pltpu.get_barrier_semaphore()
    for o in others:
        pl.semaphore_signal(barrier, inc=1, device_id=at(*o), device_id_type=MESH)

    lane = lax.broadcasted_iota(jnp.int32, (ROWS, LANES), 1)
    row = lax.broadcasted_iota(jnp.int32, (ROWS, LANES), 0)
    pick = lax.broadcasted_iota(jnp.int32, (1, LANES), 1)

    def third(b):
        position = lax.rem(lane - 108 * b + 2 * LANES * 2, LANES)
        within = position - (position // WIDE) * WIDE
        return within < EDGE, within < 2 * EDGE

    zone = [third(b) for b in range(3)]
    packed = (row < EDGE) & (lane < EDGE * WIDE)

    def gather3(ref, comps):
        out = jnp.zeros((ROWS, LANES), f32)
        for y in range(EDGE):
            for c in range(comps):
                part = ref[:, y, c, :] if comps == 3 else ref[:, y, :]
                part = jnp.concatenate([part, jnp.zeros((EDGE, LANES - EDGE), f32)], axis=1)
                part = jnp.concatenate([part, jnp.zeros((ROWS - EDGE, LANES), f32)], axis=0)
                out = out + roll(part, y * WIDE + c * EDGE)
        return out

    field, jit = gather3(field_ref, 3), gather3(jit_ref, 3) * site_spacing
    pol0 = gather3(pol_ref, 1)
    polp = pol0 + roll(pol0, EDGE) + roll(pol0, 2 * EDGE)
    weight = jnp.where(packed, 1.0 / jnp.where(packed, polp, 1.0), 0.0)
    x = polp * field

    slots = nb_ref.shape[3]
    plane = lax.broadcasted_iota(jnp.int32, (EDGE, slots), 0) * 100
    spread = [jnp.zeros((ROWS, LANES), f32) for _ in range(3)]
    for y in range(EDGE):
        for z in range(EDGE):
            entry = nb_ref[:, y, z, :]
            code = entry - plane - (222 + 10 * y + z)
            real = code > 0
            code = code + 22
            dx = jnp.where(code >= 200, 2, jnp.where(code >= 100, 1, 0))
            rem = code - dx * 100
            bit = rem - 5 * ((rem * 205) >> 11) - 2
            value = jnp.where(real, jnp.left_shift(1, jnp.where(real, bit, 0)), 0).astype(f32)
            for k in range(3):
                total = jnp.sum(jnp.where(dx == k, value, 0.0), axis=1, keepdims=True)
                total = jnp.concatenate([total, jnp.zeros((ROWS - EDGE, 1), f32)], axis=0)
                spread[k] = spread[k] + jnp.where(lane == y * WIDE + k * EDGE + z, total, 0.0)
    bits = [s.astype(jnp.int32) for s in spread]
    moved = {}

    def flag_tile(n):
        out = jnp.zeros((ROWS, LANES), jnp.int32)
        for d, (c, m) in FLAGS.items():
            if m == n:
                key = (d[0], c)
                if key not in moved:
                    moved[key] = roll(bits[d[0]], (c - d[0]) * EDGE)
                out = out | (lax.shift_right_logical(moved[key], 5 * (d[1] + 2) + d[2]) & 1)
        return out.astype(f32)

    send0[0] = jit
    send0[1] = x
    send0[2] = pol0 + flag_tile(FLAG_TILES)
    for n in range(FLAG_TILES):
        send0[3 + n] = flag_tile(n)
    own = 4
    recv0[own] = send0[...]

    def halo_start(index, src, dst):
        copies = []
        for oy in (-1, 1, 0):
            for oz in (-1, 1, 0):
                for ox in (1, 0):
                    if (ox, oy, oz) == (0, 0, 0):
                        continue
                    back = ox * 9 + (1 - oy) * 3 + 1 - oz
                    here = ox * 9 + (1 + oy) * 3 + 1 + oz
                    copies.append(
                        pltpu.make_async_remote_copy(
                            src_ref=src, dst_ref=dst.at[back],
                            send_sem=halo_send.at[index, here], recv_sem=halo_recv.at[index, back],
                            device_id=at(ox, oy, oz), device_id_type=MESH,
                        )
                    )
        for copy in copies:
            copy.start()
        return copies

    def assemble(get, c, target, fill=0.0):
        full = []
        for h in range(2):
            part = []
            for b in range(3):
                m = [roll(get(h * 9 + b * 3 + k), 108 * b + EDGE * (k - c)) for k in range(3)]
                part.append(jnp.where(zone[b][0], m[0], jnp.where(zone[b][1], m[1], m[2])))
            full.append((
                jnp.where(lane < 108, part[0], part[1]),
                jnp.where(lane < 88, part[1], part[2]),
                jnp.where(lane < 68, part[2], fill),
            ))
        for t in range(3):
            target[t, 2:8, :] = full[0][t][:6]
            target[t, 8:14, :] = full[1][t][:6]
            target[t, 0:2, :] = full[1][t][4:6]
            target[t, 14:16, :] = full[0][t][:2]

    def wide_shift(get, put):
        for half in range(2):
            rows = pl.ds(8 * half, 8)
            v = [get(t, rows) for t in range(3)]
            for i, (dy, dz) in enumerate(SHIFTS):
                a = ORIGIN + dy * WIDE + dz
                r = [roll(u, -a) for u in v]
                for t in range(2):
                    put(i, t, rows, jnp.where(lane < LANES - a, r[t], r[t + 1]))

    def near_shift(get, put):
        for half in range(2):
            rows = pl.ds(8 * half, 8)
            v = [get(t, rows) for t in range(2)]
            for i, (dy, dz) in enumerate(SHIFTS):
                s = dy * WIDE + dz
                r = [roll(u, -s) for u in v]
                if s > 0:
                    r[0] = jnp.where(lane < LANES - s, r[0], r[1])
                elif s < 0:
                    r[1] = jnp.where(lane >= -s, r[1], r[0])
                for t in range(2):
                    put(i, t, rows, r[t])

    def apply(source, target, last):
        def shift(k, carry):
            def put(i, t, rows, value):
                sh[i, t, k, rows, :] = value

            if source is None:
                wide_shift(lambda t, rows: ext[k, t, rows, :], put)
            else:
                near_shift(lambda t, rows: chain[source, k, t, rows, :], put)
            return carry

        lax.fori_loop(0, 3, shift, 0)

        def tile(t, carry):
            for rt in range(1 if last else 2):
                acc = [[None, None] for _ in range(3)]
                for i in range(len(SHIFTS)):
                    for j, dx in enumerate(SPAN[i]):
                        n = FIRST[i] + j
                        a, b, c = [sh[i, t, k, pl.ds(dx + 2 + 4 * rt, 8), :] for k in range(3)]
                        xx, xy, xz, yy, yz, zz = [coef[t, rt, n, k] for k in range(6)]
                        for k, term in enumerate((
                            xx * a + xy * b + xz * c, xy * a + yy * b + yz * c, xz * a + yz * b + zz * c,
                        )):
                            old = acc[k][n % 2]
                            acc[k][n % 2] = term if old is None else old + term
                scale = polo[t, pl.ds(2 + 4 * rt, 8), :]
                for k in range(3):
                    out = (acc[k][0] + acc[k][1]) * scale
                    chain[target, k, t, pl.ds(2 + 4 * rt, 8), :] = out
                    if not last:
                        if rt == 0:
                            chain[target, k, t, 14:16, :] = out[0:2]
                        else:
                            chain[target, k, t, 0:2, :] = out[6:8]
            return carry

        lax.fori_loop(0, 2, tile, 0)

    def pack(index):
        parts = []
        for k in range(3):
            a = OWN - EDGE * k
            r = [roll(chain[index, k, t, 2:10, :], -a) for t in range(2)]
            parts.append(jnp.where(lane < LANES - a, r[0], r[1]))
        out = jnp.where(zone[0][0], parts[0], jnp.where(zone[0][1], parts[1], parts[2]))
        return jnp.where(packed, out, 0.0)

    pl.semaphore_wait(barrier, len(others))
    copies0 = halo_start(0, send0, recv0)
    chain[...] = jnp.zeros_like(chain)
    for copy in copies0:
        copy.wait_recv()

    for k in range(3):
        assemble(lambda b: recv0[b, 0], k, geo.at[k])
        assemble(lambda b: recv0[b, 1], k, ext.at[k])
    assemble(lambda b: recv0[b, 2], 0, geo.at[4], 1.0)
    geo[3] = lax.rsqrt(geo[4])
    flagged = [
        jnp.where(zone[0][0], 0.0, recv0[b, 2]) * float(2 ** FLAG_TILES) for b in range(18)
    ]
    for n in range(FLAG_TILES):
        for b in range(18):
            flagged[b] = flagged[b] + recv0[b, 3 + n] * float(2 ** n)
    for b in range(18):
        state[0, b] = flagged[b]
    for k in range(3):
        assemble(lambda b: state[0, b], k, words.at[k])

    def shift_geo(k, carry):
        def put(i, t, rows, value):
            sgeo[i, t, k, rows, :] = value

        wide_shift(lambda t, rows: geo[k, t, rows, :], put)
        return carry

    lax.fori_loop(0, 4, shift_geo, 0)

    def shift_words(k, carry):
        def put(i, t, rows, value):
            sword[i, t, k, rows, :] = value.astype(jnp.int32)

        wide_shift(lambda t, rows: words[k, t, rows, :], put)
        return carry

    lax.fori_loop(0, 3, shift_words, 0)
    for half in range(2):
        rows = pl.ds(8 * half, 8)
        r = [roll(geo[4, t, rows, :], -ORIGIN) for t in range(3)]
        for t in range(2):
            polo[t, rows, :] = jnp.where(lane < LANES - ORIGIN, r[t], r[t + 1])

    def geometry(t, carry):
        for rt in range(2):
            base = 2 + 4 * rt
            here = [sgeo[HOME, t, k, pl.ds(base, 8), :] for k in range(4)]
            flags = [sword[HOME, t, k, pl.ds(base, 8), :] for k in range(3)]
            damped = here[3] * thole_damping
            for i, s in enumerate(SHIFTS):
                for j, dx in enumerate(SPAN[i]):
                    n = FIRST[i] + j
                    d = (dx, *s)
                    rows = pl.ds(base + dx, 8)
                    if d > (0, 0, 0):
                        c, m = FLAGS[d]
                        word = flags[c]
                    else:
                        c, m = FLAGS[tuple(-v for v in d)]
                        word = sword[i, t, c, rows, :]
                    present = (word & (1 << m)) != 0
                    sep = [
                        (sgeo[i, t, k, rows, :] - here[k]) + d[k] * site_spacing for k in range(3)
                    ]
                    sq = sep[0] * sep[0] + sep[1] * sep[1] + sep[2] * sep[2]
                    inv = lax.rsqrt(sq)
                    damp = (damped * sgeo[i, t, 3, rows, :]) * (sq * (sq * inv))
                    fall = jnp.exp(-damp)
                    inv2 = inv * inv
                    inv3 = inv2 * inv
                    iso = jnp.where(present, (1.0 - fall) * inv3, 0.0)
                    rad = jnp.where(present, (1.0 - (1.0 + damp) * fall) * (3.0 * inv3 * inv2), 0.0)
                    rs = [rad * v for v in sep]
                    coef[t, rt, n, 0] = rs[0] * sep[0] - iso
                    coef[t, rt, n, 1] = rs[0] * sep[1]
                    coef[t, rt, n, 2] = rs[0] * sep[2]
                    coef[t, rt, n, 3] = rs[1] * sep[1] - iso
                    coef[t, rt, n, 4] = rs[1] * sep[2]
                    coef[t, rt, n, 5] = rs[2] * sep[2] - iso
        return carry

    lax.fori_loop(0, 2, geometry, 0)

    def dots_start(index, vectors, number):
        line = jnp.zeros((1, LANES), f32)
        for m in range(number):
            value = weight * vectors[m // 2] * vectors[(m + 1) // 2]
            value = jnp.sum(jnp.sum(value, axis=0, keepdims=True), axis=1, keepdims=True)
            line = jnp.where(pick == m, value, line)
        dot_src[index] = line
        dot_dst[index, rank] = line
        for o in others:
            pltpu.make_async_remote_copy(
                src_ref=dot_src.at[index], dst_ref=dot_dst.at[index, rank],
                send_sem=dot_send.at[index], recv_sem=dot_recv.at[index],
                device_id=at(*o), device_id_type=MESH,
            ).start()

    def dots_all(index):
        some = dot_dst.at[index, pl.ds(0, count - 1)]
        return pltpu.make_async_remote_copy(
            src_ref=some, dst_ref=some, send_sem=dot_send.at[index], recv_sem=dot_recv.at[index],
            device_id=at(1, 0, 0), device_id_type=MESH,
        )

    def dots_finish(index, number):
        dots_all(index).wait_recv()
        line = jnp.sum(dot_dst[index, :, 0, :], axis=0, keepdims=True)
        return [
            jnp.broadcast_to(jnp.sum(jnp.where(pick == m, line, 0.0), axis=1, keepdims=True), (ROWS, LANES))
            for m in range(number)
        ]

    def scalars(moments, history, steps):
        number = 2 * steps
        before = [0.0] * number
        if history:
            _, _, mu1, eta1, inv1, _ = history[-1]
            _, _, mu2, eta2, inv2, _ = history[-2]
            before[1] = moments[0] * inv1
            before[2] = moments[1] * inv1 + mu1 * before[1]
            older2 = before[1] * inv2
            before[3] = moments[2] * inv1 + mu1 * before[2] + eta1 * older2
            older3 = before[2] * inv2 + mu2 * older2
            before[4] = moments[3] * inv1 + mu1 * before[3] + eta1 * older3
        now, lead, seen = list(moments), None, 0.0
        out = []
        known = list(history)
        for i in range(steps):
            gamma = now[i] if lead is None else lead * now[i]
            if known:
                eta = gamma * known[-1][4] / known[-1][5]
                beta = eta * known[-1][0]
            else:
                eta = beta = jnp.zeros((ROWS, LANES), f32)
            ratio = now[i + 1] / now[i]
            mu = ratio - seen
            seen = ratio
            inv = 1.0 - mu - eta
            alpha = 1.0 / inv
            later = [0.0] * number
            for m in range(i + 1, number - 1 - i):
                later[m] = alpha * (now[m + 1] - mu * now[m] - eta * before[m])
            before, now = now, later
            lead = alpha if lead is None else lead * alpha
            out.append((alpha, beta, mu, eta, inv, gamma))
            known.append(out[-1])
        return out

    def advance(values, old, cs, history):
        zm, cm, cmm = old
        (a0, _, m0, e0, _, _), (a1, _, m1, e1, _, _) = cs[:2]
        z0, v1, v2 = values[:3]
        if zm is None:
            z1 = a0 * (v1 - m0 * z0)
            c1 = a0 * (v2 - m0 * v1)
        else:
            z1 = a0 * (v1 - m0 * z0 - e0 * zm)
            c1 = a0 * (v2 - m0 * v1 - e0 * cm)
        z2 = a1 * (c1 - m1 * z1 - e1 * z0)
        if len(cs) == 2:
            return [z1, z2], (z1, c1, v1)
        v3 = values[3]
        a2, _, m2, e2, _, _ = cs[2]
        _, _, mu1, eta1, inv1, _ = history[-1]
        ccm = v1 * inv1 + mu1 * cm + eta1 * cmm
        cc1 = a0 * (v3 - m0 * v2 - e0 * ccm)
        c2 = a1 * (cc1 - m1 * c1 - e1 * v1)
        z3 = a2 * (c2 - m2 * z2 - e2 * z1)
        return [z1, z2, z3], (z2, c2, c1)

    line = jnp.zeros((1, LANES), f32)
    history = []
    pending = []
    p = None
    for index, steps in enumerate(BLOCKS):
        final = index == len(BLOCKS) - 1
        if index == 0:
            apply(None, 0, False)
            apply(0, 1, False)
            apply(1, 2, True)
            mine = [pack(0), pack(1), pack(2)]
            sent = mine
        else:
            apply(None, 1, False)
            apply(1, 2, False)
            apply(2, 3, True)
            mine = [z, pack(1), pack(2), pack(3)]
            sent = mine[1:]
        dots_start(index, mine, 2 * steps)
        if not final:
            for k in range(3):
                send1[index, k] = sent[k]
                recv1[index, own, k] = sent[k]
            copies = halo_start(1 + index, send1.at[index], recv1.at[index])
            pending.append(copies)
            for copy in copies:
                copy.wait_recv()
        moments = dots_finish(index, 2 * steps)
        cs = scalars(moments, history, steps)
        if not final:
            for b in range(18):
                got = [recv1[index, b, k] for k in range(3)]
                if index == 0:
                    values, old = got, (None, None, None)
                else:
                    values = [state[0, b], *got]
                    old = (state[1, b], state[2, b], state[3, b])
                zs, new = advance(values, old, cs, history)
                if b == own:
                    mine_z = zs
                    z_start = values[0]
                state[0, b] = zs[-1]
                for k in range(3):
                    state[1 + k, b] = new[k]
            for k in range(3):
                assemble(lambda b: state[0, b], k, ext.at[k])
            z = mine_z[-1]
        else:
            mine_z, _ = advance(mine, (state[1, own], state[2, own], state[3, own]), cs, history)
            z_start = mine[0]
        for i in range(steps):
            before = z_start if i == 0 else mine_z[i - 1]
            alpha, beta = cs[i][0], cs[i][1]
            p = before if p is None else before + beta * p
            x = x + alpha * p
            line = jnp.where(pick == len(history) + i, alpha[0:1], line)
        history = history + cs

    residual = mine_z[-1] * weight
    for y in range(EDGE):
        for c in range(3):
            shift = -(y * WIDE + c * EDGE)
            x_out[:, y, c, :] = roll(x, shift)[:EDGE, :EDGE]
            r_out[:, y, c, :] = roll(residual, shift)[:EDGE, :EDGE]
    len_out[...] = line

    for copy in copies0:
        copy.wait_send()
    for copies in pending:
        for copy in copies:
            copy.wait_send()
    for index in range(len(BLOCKS)):
        dots_all(index).wait_send()


def solution(mesh):
    sizes = tuple(mesh.shape[a] for a in ("gx", "gy", "gz"))
    assert sizes[0] == 2
    count = sizes[0] * sizes[1] * sizes[2]

    def local(permanent_field, polar, jitter, neighbors):
        assert polar.shape == (EDGE, EDGE, EDGE)
        vmem = pl.BlockSpec(memory_space=pltpu.VMEM)
        shape = jax.ShapeDtypeStruct((EDGE, EDGE, 3, EDGE), f32)
        wide, near = (3, 16, LANES), (2, 16, LANES)
        shifts = len(SHIFTS)
        x, r, steps = pl.pallas_call(
            functools.partial(kernel, sizes),
            out_shape=(shape, shape, jax.ShapeDtypeStruct((1, LANES), f32)),
            in_specs=[vmem] * 4,
            out_specs=(vmem, vmem, vmem),
            scratch_shapes=[
                pltpu.VMEM((3, *wide), f32),
                pltpu.VMEM((shifts, 2, 3, 16, LANES), f32),
                pltpu.VMEM((5, *wide), f32),
                pltpu.VMEM((3, *wide), f32),
                pltpu.VMEM((shifts, 2, 4, 16, LANES), f32),
                pltpu.VMEM((shifts, 2, 3, 16, LANES), jnp.int32),
                pltpu.VMEM(near, f32),
                pltpu.VMEM((2, 2, len(STENCIL), 6, ROWS, LANES), f32),
                pltpu.VMEM((4, 3, *near), f32),
                pltpu.VMEM((4, 18, ROWS, LANES), f32),
                pltpu.VMEM((TILES, ROWS, LANES), f32),
                pltpu.VMEM((18, TILES, ROWS, LANES), f32),
                pltpu.VMEM((2, 3, ROWS, LANES), f32),
                pltpu.VMEM((2, 18, 3, ROWS, LANES), f32),
                pltpu.VMEM((3, 1, LANES), f32),
                pltpu.VMEM((3, count, 1, LANES), f32),
                pltpu.SemaphoreType.DMA((3, 18)),
                pltpu.SemaphoreType.DMA((3, 18)),
                pltpu.SemaphoreType.DMA((3,)),
                pltpu.SemaphoreType.DMA((3,)),
            ],
            compiler_params=pltpu.CompilerParams(collective_id=0, has_side_effects=True),
        )(
            jnp.moveaxis(permanent_field, -1, 2),
            polar,
            jnp.moveaxis(jitter, -1, 2),
            neighbors,
        )
        return jnp.moveaxis(x, 2, -1), jnp.moveaxis(r, 2, -1), steps[0, :ITERS]

    return jax.shard_map(
        local,
        mesh=mesh,
        in_specs=(
            P("gx", "gy", "gz", None),
            P("gx", "gy", "gz"),
            P("gx", "gy", "gz", None),
            P("gx", "gy", "gz", None),
        ),
        out_specs=(P("gx", "gy", "gz", None), P("gx", "gy", "gz", None), P()),
        check_vma=False,
    )
```

```python
import functools

import jax
import jax.numpy as jnp
from jax import lax
from jax.experimental import pallas as pl
from jax.experimental.pallas import tpu as pltpu
from jax.sharding import PartitionSpec as P

ITERS = 8
BLOCKS = (2, 3, 3)
MESH = pl.DeviceIdType.MESH
thole_damping = 0.39
site_spacing = 3.5
ROWS, LANES = 8, 128
EDGE = 6
WIDE = 3 * EDGE
ORIGIN = 2 * WIDE + 2
OWN = EDGE * WIDE + EDGE - ORIGIN
f32 = jnp.float32

STENCIL = [
    (a, b, c)
    for a in range(-2, 3)
    for b in range(-2, 3)
    for c in range(-2, 3)
    if 1 <= a * a + b * b + c * c <= 5
]
SHIFTS = sorted({(b, c) for a, b, c in STENCIL})
SPAN = [[d[0] for d in STENCIL if d[1:] == s] for s in SHIFTS]
FIRST = [sum(len(v) for v in SPAN[:i]) for i in range(len(SHIFTS))]
HOME = SHIFTS.index((0, 0))
FORWARD = [d for d in STENCIL if d > (0, 0, 0)]


def flag_places():
    room = {0: 9, 1: 10, 2: 10}
    used = {0: 0, 1: 0, 2: 0}
    places = {}
    for d in FORWARD:
        c = d[0] if used[d[0]] < room[d[0]] else 2
        if d[0] != 2 and used[d[0]] >= room[d[0]]:
            c = 2
        places[d] = (c, used[c])
        used[c] += 1
    assert used[2] <= room[2]
    return places


FLAGS = flag_places()
FLAG_TILES = 9
TILES = 3 + FLAG_TILES


def roll(value, shift):
    shift = shift % LANES
    return value if shift == 0 else pltpu.roll(value, shift, axis=1)


def kernel(
    sizes,
    field_in, pol_in, jit_in, nb_in, out_ref,
    field_ref, pol_ref, jit_ref, nb_ref,
    ext, sh, geo, words, sgeo, sword, polo, coef, chain, state,
    send0, recv0, send1, recv1, dot_src, dot_dst,
    halo_send, halo_recv, dot_send, dot_recv, in_sems,
):
    nx, ny, nz = sizes
    count = nx * ny * nz
    gx, gy, gz = lax.axis_index("gx"), lax.axis_index("gy"), lax.axis_index("gz")
    rank = (gx * ny + gy) * nz + gz

    def at(ox, oy, oz):
        return (lax.rem(gx + ox + nx, nx), lax.rem(gy + oy + ny, ny), lax.rem(gz + oz + nz, nz))

    others = [
        (a, b, c) for a in range(nx) for b in range(ny) for c in range(nz) if (a, b, c) != (0, 0, 0)
    ]
    others.sort(key=lambda o: -(min(o[0], nx - o[0]) + 2 * min(o[1], ny - o[1]) + 2 * min(o[2], nz - o[2])))

    barrier = pltpu.get_barrier_semaphore()
    for o in others:
        pl.semaphore_signal(barrier, inc=1, device_id=at(*o), device_id_type=MESH)
    loads = [
        pltpu.make_async_copy(source, target, in_sems.at[k])
        for k, (source, target) in enumerate((
            (nb_in, nb_ref), (field_in, field_ref), (pol_in, pol_ref), (jit_in, jit_ref),
        ))
    ]
    for load in loads:
        load.start()

    lane = lax.broadcasted_iota(jnp.int32, (ROWS, LANES), 1)
    row = lax.broadcasted_iota(jnp.int32, (ROWS, LANES), 0)
    pick = lax.broadcasted_iota(jnp.int32, (1, LANES), 1)

    def third(b):
        position = lax.rem(lane - 108 * b + 2 * LANES * 2, LANES)
        within = position - (position // WIDE) * WIDE
        return within < EDGE, within < 2 * EDGE

    zone = [third(b) for b in range(3)]
    packed = (row < EDGE) & (lane < EDGE * WIDE)

    def gather3(ref, comps):
        out = jnp.zeros((ROWS, LANES), f32)
        for y in range(EDGE):
            for c in range(comps):
                part = ref[:, y, c, :] if comps == 3 else ref[:, y, :]
                part = jnp.concatenate([part, jnp.zeros((EDGE, LANES - EDGE), f32)], axis=1)
                part = jnp.concatenate([part, jnp.zeros((ROWS - EDGE, LANES), f32)], axis=0)
                out = out + roll(part, y * WIDE + c * EDGE)
        return out

    for load in loads:
        load.wait()
    field, jit = gather3(field_ref, 3), gather3(jit_ref, 3) * site_spacing
    pol0 = gather3(pol_ref, 1)
    polp = pol0 + roll(pol0, EDGE) + roll(pol0, 2 * EDGE)
    weight = jnp.where(packed, 1.0 / jnp.where(packed, polp, 1.0), 0.0)
    x = polp * field

    slots = nb_ref.shape[3]
    plane = lax.broadcasted_iota(jnp.int32, (EDGE, slots), 0) * 100
    spread = [jnp.zeros((ROWS, LANES), f32) for _ in range(3)]
    for y in range(EDGE):
        for z in range(EDGE):
            entry = nb_ref[:, y, z, :]
            code = entry - plane - (222 + 10 * y + z)
            real = code > 0
            code = code + 22
            dx = jnp.where(code >= 200, 2, jnp.where(code >= 100, 1, 0))
            rem = code - dx * 100
            bit = rem - 5 * ((rem * 205) >> 11) - 2
            value = jnp.where(real, jnp.left_shift(1, jnp.where(real, bit, 0)), 0).astype(f32)
            for k in range(3):
                total = jnp.sum(jnp.where(dx == k, value, 0.0), axis=1, keepdims=True)
                total = jnp.concatenate([total, jnp.zeros((ROWS - EDGE, 1), f32)], axis=0)
                spread[k] = spread[k] + jnp.where(lane == y * WIDE + k * EDGE + z, total, 0.0)
    bits = [s.astype(jnp.int32) for s in spread]
    moved = {}

    def flag_tile(n):
        out = jnp.zeros((ROWS, LANES), jnp.int32)
        for d, (c, m) in FLAGS.items():
            if m == n:
                key = (d[0], c)
                if key not in moved:
                    moved[key] = roll(bits[d[0]], (c - d[0]) * EDGE)
                out = out | (lax.shift_right_logical(moved[key], 5 * (d[1] + 2) + d[2]) & 1)
        return out.astype(f32)

    send0[0] = jit
    send0[1] = x
    send0[2] = pol0 + flag_tile(FLAG_TILES)
    for n in range(FLAG_TILES):
        send0[3 + n] = flag_tile(n)
    own = 4
    recv0[own] = send0[...]

    def halo_start(index, src, get_dst):
        copies = []
        for oy in (-1, 1, 0):
            for oz in (-1, 1, 0):
                for ox in (1, 0):
                    if (ox, oy, oz) == (0, 0, 0):
                        continue
                    back = ox * 9 + (1 - oy) * 3 + 1 - oz
                    here = ox * 9 + (1 + oy) * 3 + 1 + oz
                    copies.append(
                        pltpu.make_async_remote_copy(
                            src_ref=src, dst_ref=get_dst(back),
                            send_sem=halo_send.at[index, here], recv_sem=halo_recv.at[index, back],
                            device_id=at(ox, oy, oz), device_id_type=MESH,
                        )
                    )
        for copy in copies:
            copy.start()
        return copies

    def assemble(get, c, target, fill=0.0):
        full = []
        for h in range(2):
            part = []
            for b in range(3):
                m = [roll(get(h * 9 + b * 3 + k), 108 * b + EDGE * (k - c)) for k in range(3)]
                part.append(jnp.where(zone[b][0], m[0], jnp.where(zone[b][1], m[1], m[2])))
            full.append((
                jnp.where(lane < 108, part[0], part[1]),
                jnp.where(lane < 88, part[1], part[2]),
                jnp.where(lane < 68, part[2], fill),
            ))
        for t in range(3):
            target[t, 2:8, :] = full[0][t][:6]
            target[t, 8:14, :] = full[1][t][:6]
            target[t, 0:2, :] = full[1][t][4:6]
            target[t, 14:16, :] = full[0][t][:2]

    def shifted(v, i):
        dy, dz = SHIFTS[i]
        s = dy * WIDE + dz + (ORIGIN if len(v) == 3 else 0)
        if s == 0:
            return v
        r = [roll(u, -s) for u in v]
        if len(v) == 3:
            return [jnp.where(lane < LANES - s, r[t], r[t + 1]) for t in range(2)]
        if s > 0:
            return [jnp.where(lane < LANES - s, r[0], r[1]), r[1]]
        return [r[0], jnp.where(lane >= -s, r[1], r[0])]

    halves = (pl.ds(0, 8), pl.ds(8, 8))

    def apply(source, target, last):
        tiles = range(3) if source is None else range(2)

        def shift(i):
            for k in range(3):
                for rows in halves:
                    ref = ext.at[k] if source is None else chain.at[source, k]
                    for t, value in enumerate(shifted([ref[t, rows, :] for t in tiles], i)):
                        sh[i, t, k, rows, :] = value

        sides = [(t, rt) for t in range(2) for rt in range(1 if last else 2)]
        acc = {side: [None] * 3 for side in sides}

        def compute(i):
            for j, dx in enumerate(SPAN[i]):
                n = FIRST[i] + j
                for t, rt in sides:
                    v = [sh[i, t, k, pl.ds(dx + 2 + 4 * rt, 8), :] for k in range(3)]
                    u = [coef[t, rt, n, k] for k in range(3)]
                    iso = coef[t, rt, n, 3]
                    dot = u[0] * v[0] + u[1] * v[1] + u[2] * v[2]
                    for k in range(3):
                        term = u[k] * dot - iso * v[k]
                        old = acc[t, rt][k]
                        acc[t, rt][k] = term if old is None else old + term

        ahead = 4
        for i in range(len(SHIFTS) + ahead):
            if i < len(SHIFTS):
                shift(i)
            if i >= ahead:
                compute(i - ahead)
        for t, rt in sides:
            scale = polo[t, pl.ds(2 + 4 * rt, 8), :]
            for k in range(3):
                out = acc[t, rt][k] * scale
                chain[target, k, t, pl.ds(2 + 4 * rt, 8), :] = out
                if not last:
                    if rt == 0:
                        chain[target, k, t, 14:16, :] = out[0:2]
                    else:
                        chain[target, k, t, 0:2, :] = out[6:8]

    def pack(index):
        parts = []
        for k in range(3):
            a = OWN - EDGE * k
            r = [roll(chain[index, k, t, 2:10, :], -a) for t in range(2)]
            parts.append(jnp.where(lane < LANES - a, r[0], r[1]))
        out = jnp.where(zone[0][0], parts[0], jnp.where(zone[0][1], parts[1], parts[2]))
        return jnp.where(packed, out, 0.0)

    pl.semaphore_wait(barrier, len(others))
    copies0 = halo_start(0, send0, lambda b: recv0.at[b])
    chain[...] = jnp.zeros_like(chain)
    for copy in copies0:
        copy.wait_recv()

    for k in range(3):
        assemble(lambda b: recv0[b, 0], k, geo.at[k])
        assemble(lambda b: recv0[b, 1], k, ext.at[k])
    assemble(lambda b: recv0[b, 2], 0, geo.at[4], 1.0)
    geo[3] = lax.rsqrt(geo[4])
    flagged = [
        jnp.where(zone[0][0], 0.0, recv0[b, 2]) * float(2 ** FLAG_TILES) for b in range(18)
    ]
    for n in range(FLAG_TILES):
        for b in range(18):
            flagged[b] = flagged[b] + recv0[b, 3 + n] * float(2 ** n)
    for b in range(18):
        state[0, b] = flagged[b]
    for k in range(3):
        assemble(lambda b: state[0, b], k, words.at[k])

    for i in range(len(SHIFTS)):
        for rows in halves:
            for k in range(4):
                for t, value in enumerate(shifted([geo[k, t, rows, :] for t in range(3)], i)):
                    sgeo[i, t, k, rows, :] = value
            for k in range(3):
                for t, value in enumerate(shifted([words[k, t, rows, :] for t in range(3)], i)):
                    sword[i, t, k, rows, :] = value.astype(jnp.int32)
    for half in range(2):
        rows = pl.ds(8 * half, 8)
        r = [roll(geo[4, t, rows, :], -ORIGIN) for t in range(3)]
        for t in range(2):
            polo[t, rows, :] = jnp.where(lane < LANES - ORIGIN, r[t], r[t + 1])

    def geometry(t, carry):
        for rt in range(2):
            base = 2 + 4 * rt
            here = [sgeo[HOME, t, k, pl.ds(base, 8), :] for k in range(4)]
            flags = [sword[HOME, t, k, pl.ds(base, 8), :] for k in range(3)]
            damped = here[3] * thole_damping
            for i, s in enumerate(SHIFTS):
                for j, dx in enumerate(SPAN[i]):
                    n = FIRST[i] + j
                    d = (dx, *s)
                    rows = pl.ds(base + dx, 8)
                    if d > (0, 0, 0):
                        c, m = FLAGS[d]
                        word = flags[c]
                    else:
                        c, m = FLAGS[tuple(-v for v in d)]
                        word = sword[i, t, c, rows, :]
                    present = (word & (1 << m)) != 0
                    sep = [sgeo[i, t, k, rows, :] - here[k] for k in range(3)]
                    sep = [v + e * site_spacing if e else v for v, e in zip(sep, d)]
                    sq = sep[0] * sep[0] + sep[1] * sep[1] + sep[2] * sep[2]
                    inv = lax.rsqrt(sq)
                    damp = (damped * sgeo[i, t, 3, rows, :]) * (sq * (sq * inv))
                    fall = jnp.exp(-damp)
                    inv2 = inv * inv
                    inv3 = inv2 * inv
                    iso = jnp.where(present, (1.0 - fall) * inv3, 0.0)
                    rad = (1.0 - (1.0 + damp) * fall) * (3.0 * inv3 * inv2)
                    root = jnp.where(present, rad * lax.rsqrt(rad), 0.0)
                    for k in range(3):
                        coef[t, rt, n, k] = root * sep[k]
                    coef[t, rt, n, 3] = iso
        return carry

    lax.fori_loop(0, 2, geometry, 0)

    def dots_start(index, vectors, number):
        line = jnp.zeros((1, LANES), f32)
        for m in range(number):
            value = weight * vectors[m // 2] * vectors[(m + 1) // 2]
            value = jnp.sum(jnp.sum(value, axis=0, keepdims=True), axis=1, keepdims=True)
            line = jnp.where(pick == m, value, line)
        dot_src[index] = line
        dot_dst[index, rank] = line
        for o in others:
            pltpu.make_async_remote_copy(
                src_ref=dot_src.at[index], dst_ref=dot_dst.at[index, rank],
                send_sem=dot_send.at[index], recv_sem=dot_recv.at[index],
                device_id=at(*o), device_id_type=MESH,
            ).start()

    def dots_all(index):
        some = dot_dst.at[index, pl.ds(0, count - 1)]
        return pltpu.make_async_remote_copy(
            src_ref=some, dst_ref=some, send_sem=dot_send.at[index], recv_sem=dot_recv.at[index],
            device_id=at(1, 0, 0), device_id_type=MESH,
        )

    def dots_finish(index, number):
        dots_all(index).wait_recv()
        line = jnp.sum(dot_dst[index, :, 0, :], axis=0, keepdims=True)
        return [
            jnp.broadcast_to(jnp.sum(jnp.where(pick == m, line, 0.0), axis=1, keepdims=True), (ROWS, LANES))
            for m in range(number)
        ]

    def scalars(moments, history, steps):
        number = 2 * steps
        before = [0.0] * number
        if history:
            _, _, mu1, eta1, inv1, _ = history[-1]
            _, _, mu2, eta2, inv2, _ = history[-2]
            before[1] = moments[0] * inv1
            before[2] = moments[1] * inv1 + mu1 * before[1]
            older2 = before[1] * inv2
            before[3] = moments[2] * inv1 + mu1 * before[2] + eta1 * older2
            older3 = before[2] * inv2 + mu2 * older2
            before[4] = moments[3] * inv1 + mu1 * before[3] + eta1 * older3
        now, lead, seen = list(moments), None, 0.0
        out = []
        known = list(history)
        for i in range(steps):
            gamma = now[i] if lead is None else lead * now[i]
            if known:
                eta = gamma * known[-1][4] / known[-1][5]
                beta = eta * known[-1][0]
            else:
                eta = beta = jnp.zeros((ROWS, LANES), f32)
            ratio = now[i + 1] / now[i]
            mu = ratio - seen
            seen = ratio
            inv = 1.0 - mu - eta
            alpha = 1.0 / inv
            later = [0.0] * number
            for m in range(i + 1, number - 1 - i):
                later[m] = alpha * (now[m + 1] - mu * now[m] - eta * before[m])
            before, now = now, later
            lead = alpha if lead is None else lead * alpha
            out.append((alpha, beta, mu, eta, inv, gamma))
            known.append(out[-1])
        return out

    def advance(values, old, cs, history):
        zm, cm, cmm = old
        (a0, _, m0, e0, _, _), (a1, _, m1, e1, _, _) = cs[:2]
        z0, v1, v2 = values[:3]
        if zm is None:
            z1 = a0 * (v1 - m0 * z0)
            c1 = a0 * (v2 - m0 * v1)
        else:
            z1 = a0 * (v1 - m0 * z0 - e0 * zm)
            c1 = a0 * (v2 - m0 * v1 - e0 * cm)
        z2 = a1 * (c1 - m1 * z1 - e1 * z0)
        if len(cs) == 2:
            return [z1, z2], (z1, c1, v1)
        v3 = values[3]
        a2, _, m2, e2, _, _ = cs[2]
        _, _, mu1, eta1, inv1, _ = history[-1]
        ccm = v1 * inv1 + mu1 * cm + eta1 * cmm
        cc1 = a0 * (v3 - m0 * v2 - e0 * ccm)
        c2 = a1 * (cc1 - m1 * c1 - e1 * v1)
        z3 = a2 * (c2 - m2 * z2 - e2 * z1)
        return [z1, z2, z3], (z2, c2, c1)

    line = jnp.zeros((1, LANES), f32)
    history = []
    pending = []
    p = None
    for index, steps in enumerate(BLOCKS):
        final = index == len(BLOCKS) - 1
        copies = []

        def share(k, value):
            if not final:
                send1[index, k] = value
                recv1[index, own, k] = value
                copies.extend(halo_start(
                    1 + 3 * index + k, send1.at[index, k], lambda b: recv1.at[index, b, k]
                ))
            return value

        start = 0 if index == 0 else 1
        mine = [] if index == 0 else [z]
        for k in range(3):
            apply(None if k == 0 else start + k - 1, start + k, k == 2)
            mine.append(share(k, pack(start + k)))
        dots_start(index, mine, 2 * steps)
        pending.append(copies)
        for copy in copies:
            copy.wait_recv()
        moments = dots_finish(index, 2 * steps)
        cs = scalars(moments, history, steps)
        if not final:
            for b in range(18):
                got = [recv1[index, b, k] for k in range(3)]
                if index == 0:
                    values, old = got, (None, None, None)
                else:
                    values = [state[0, b], *got]
                    old = (state[1, b], state[2, b], state[3, b])
                zs, new = advance(values, old, cs, history)
                if b == own:
                    mine_z = zs
                    z_start = values[0]
                state[0, b] = zs[-1]
                for k in range(3):
                    state[1 + k, b] = new[k]
            for k in range(3):
                assemble(lambda b: state[0, b], k, ext.at[k])
            z = mine_z[-1]
        else:
            mine_z, _ = advance(mine, (state[1, own], state[2, own], state[3, own]), cs, history)
            z_start = mine[0]
        for i in range(steps):
            before = z_start if i == 0 else mine_z[i - 1]
            alpha, beta = cs[i][0], cs[i][1]
            p = before if p is None else before + beta * p
            x = x + alpha * p
            line = jnp.where(pick == len(history) + i, alpha[0:1], line)
        history = history + cs

    residual = mine_z[-1] * weight
    out_ref[0] = x
    out_ref[1] = residual
    out_ref[2, 0:1, :] = line

    for copy in copies0:
        copy.wait_send()
    for copies in pending:
        for copy in copies:
            copy.wait_send()
    for index in range(len(BLOCKS)):
        dots_all(index).wait_send()


def unpack(in_ref, x_out, r_out, len_out):
    for k, ref in enumerate((x_out, r_out)):
        value = in_ref[k]
        for y in range(EDGE):
            for c in range(3):
                ref[:, y, c, :] = roll(value, -(y * WIDE + c * EDGE))[:EDGE, :EDGE]
    len_out[...] = in_ref[2, 0:1, :ITERS]


def solution(mesh):
    sizes = tuple(mesh.shape[a] for a in ("gx", "gy", "gz"))
    assert sizes[0] == 2
    count = sizes[0] * sizes[1] * sizes[2]

    def local(permanent_field, polar, jitter, neighbors):
        assert polar.shape == (EDGE, EDGE, EDGE)
        vmem = pl.BlockSpec(memory_space=pltpu.VMEM)
        shape = jax.ShapeDtypeStruct((EDGE, EDGE, 3, EDGE), f32)
        wide, near = (3, 16, LANES), (2, 16, LANES)
        shifts = len(SHIFTS)
        anywhere = pl.BlockSpec(memory_space=pl.ANY)
        packed = pl.pallas_call(
            functools.partial(kernel, sizes),
            out_shape=jax.ShapeDtypeStruct((3, ROWS, LANES), f32),
            in_specs=[anywhere] * 4,
            out_specs=vmem,
            scratch_shapes=[
                pltpu.VMEM((EDGE, EDGE, 3, EDGE), f32),
                pltpu.VMEM((EDGE, EDGE, EDGE), f32),
                pltpu.VMEM((EDGE, EDGE, 3, EDGE), f32),
                pltpu.VMEM(neighbors.shape, jnp.int32),
                pltpu.VMEM((3, *wide), f32),
                pltpu.VMEM((shifts, 2, 3, 16, LANES), f32),
                pltpu.VMEM((5, *wide), f32),
                pltpu.VMEM((3, *wide), f32),
                pltpu.VMEM((shifts, 2, 4, 16, LANES), f32),
                pltpu.VMEM((shifts, 2, 3, 16, LANES), jnp.int32),
                pltpu.VMEM(near, f32),
                pltpu.VMEM((2, 2, len(STENCIL), 4, ROWS, LANES), f32),
                pltpu.VMEM((4, 3, *near), f32),
                pltpu.VMEM((4, 18, ROWS, LANES), f32),
                pltpu.VMEM((TILES, ROWS, LANES), f32),
                pltpu.VMEM((18, TILES, ROWS, LANES), f32),
                pltpu.VMEM((2, 3, ROWS, LANES), f32),
                pltpu.VMEM((2, 18, 3, ROWS, LANES), f32),
                pltpu.VMEM((3, 1, LANES), f32),
                pltpu.VMEM((3, count, 1, LANES), f32),
                pltpu.SemaphoreType.DMA((7, 18)),
                pltpu.SemaphoreType.DMA((7, 18)),
                pltpu.SemaphoreType.DMA((3,)),
                pltpu.SemaphoreType.DMA((3,)),
                pltpu.SemaphoreType.DMA((4,)),
            ],
            compiler_params=pltpu.CompilerParams(collective_id=0, has_side_effects=True),
        )(
            jnp.moveaxis(permanent_field, -1, 2),
            polar,
            jnp.moveaxis(jitter, -1, 2),
            neighbors,
        )
        x, r, steps = pl.pallas_call(
            unpack,
            out_shape=(shape, shape, jax.ShapeDtypeStruct((1, ITERS), f32)),
            in_specs=[vmem],
            out_specs=(vmem, vmem, vmem),
        )(packed)
        return jnp.moveaxis(x, 2, -1), jnp.moveaxis(r, 2, -1), steps.reshape(ITERS)

    return jax.shard_map(
        local,
        mesh=mesh,
        in_specs=(
            P("gx", "gy", "gz", None),
            P("gx", "gy", "gz"),
            P("gx", "gy", "gz", None),
            P("gx", "gy", "gz", None),
        ),
        out_specs=(P("gx", "gy", "gz", None), P("gx", "gy", "gz", None), P()),
        check_vma=False,
    )
```

```python
import functools

import jax
import jax.numpy as jnp
from jax import lax
from jax.experimental import pallas as pl
from jax.experimental.pallas import tpu as pltpu
from jax.sharding import PartitionSpec as P

ITERS = 8
MESH = pl.DeviceIdType.MESH
thole_damping = 0.39
site_spacing = 3.5
ROWS, LANES = 8, 128
EDGE = 6
WIDE = 3 * EDGE
ORIGIN = 2 * WIDE + 2
OWN = EDGE * WIDE + EDGE - ORIGIN
f32 = jnp.float32

STENCIL = [
    (a, b, c)
    for a in range(-2, 3)
    for b in range(-2, 3)
    for c in range(-2, 3)
    if 1 <= a * a + b * b + c * c <= 5
]
SHIFTS = sorted({(b, c) for a, b, c in STENCIL})
SPAN = [[d[0] for d in STENCIL if d[1:] == s] for s in SHIFTS]
FIRST = [sum(len(v) for v in SPAN[:i]) for i in range(len(SHIFTS))]
HOME = SHIFTS.index((0, 0))
FORWARD = [d for d in STENCIL if d > (0, 0, 0)]


def flag_places():
    room = {0: 9, 1: 10, 2: 10}
    used = {0: 0, 1: 0, 2: 0}
    places = {}
    for d in FORWARD:
        c = d[0] if used[d[0]] < room[d[0]] else 2
        if d[0] != 2 and used[d[0]] >= room[d[0]]:
            c = 2
        places[d] = (c, used[c])
        used[c] += 1
    assert used[2] <= room[2]
    return places


FLAGS = flag_places()
FLAG_TILES = 9
TILES = 3 + FLAG_TILES


def roll(value, shift):
    shift = shift % LANES
    return value if shift == 0 else pltpu.roll(value, shift, axis=1)


def kernel(
    sizes,
    field_in, pol_in, jit_in, nb_in, out_ref,
    field_ref, pol_ref, jit_ref, nb_ref,
    ext, sh, geo, words, sgeo, sword, polo, coef, chain,
    send0, recv0, send1, recv1, dot_src, dot_dst,
    halo_send, halo_recv, dot_send, dot_recv, in_sems,
):
    nx, ny, nz = sizes
    count = nx * ny * nz
    gx, gy, gz = lax.axis_index("gx"), lax.axis_index("gy"), lax.axis_index("gz")
    rank = (gx * ny + gy) * nz + gz

    def at(ox, oy, oz):
        return (lax.rem(gx + ox + nx, nx), lax.rem(gy + oy + ny, ny), lax.rem(gz + oz + nz, nz))

    others = [
        (a, b, c) for a in range(nx) for b in range(ny) for c in range(nz) if (a, b, c) != (0, 0, 0)
    ]
    others.sort(key=lambda o: -(min(o[0], nx - o[0]) + 2 * min(o[1], ny - o[1]) + 2 * min(o[2], nz - o[2])))

    barrier = pltpu.get_barrier_semaphore()
    for o in others:
        pl.semaphore_signal(barrier, inc=1, device_id=at(*o), device_id_type=MESH)
    loads = [
        pltpu.make_async_copy(source, target, in_sems.at[k])
        for k, (source, target) in enumerate((
            (nb_in, nb_ref), (field_in, field_ref), (pol_in, pol_ref), (jit_in, jit_ref),
        ))
    ]
    for load in loads:
        load.start()

    lane = lax.broadcasted_iota(jnp.int32, (ROWS, LANES), 1)
    row = lax.broadcasted_iota(jnp.int32, (ROWS, LANES), 0)
    pick = lax.broadcasted_iota(jnp.int32, (1, LANES), 1)

    def third(b):
        position = lax.rem(lane - 108 * b + 2 * LANES * 2, LANES)
        within = position - (position // WIDE) * WIDE
        return within < EDGE, within < 2 * EDGE

    zone = [third(b) for b in range(3)]
    packed = (row < EDGE) & (lane < EDGE * WIDE)

    def gather3(ref, comps):
        out = jnp.zeros((ROWS, LANES), f32)
        for y in range(EDGE):
            for c in range(comps):
                part = ref[:, y, c, :] if comps == 3 else ref[:, y, :]
                part = jnp.concatenate([part, jnp.zeros((EDGE, LANES - EDGE), f32)], axis=1)
                part = jnp.concatenate([part, jnp.zeros((ROWS - EDGE, LANES), f32)], axis=0)
                out = out + roll(part, y * WIDE + c * EDGE)
        return out

    for load in loads:
        load.wait()
    field, jit = gather3(field_ref, 3), gather3(jit_ref, 3) * site_spacing
    pol0 = gather3(pol_ref, 1)
    polp = pol0 + roll(pol0, EDGE) + roll(pol0, 2 * EDGE)
    weight = jnp.where(packed, 1.0 / jnp.where(packed, polp, 1.0), 0.0)
    x = polp * field

    slots = nb_ref.shape[3]
    plane = lax.broadcasted_iota(jnp.int32, (EDGE, slots), 0) * 100
    spread = [jnp.zeros((ROWS, LANES), f32) for _ in range(3)]
    for y in range(EDGE):
        for z in range(EDGE):
            entry = nb_ref[:, y, z, :]
            code = entry - plane - (222 + 10 * y + z)
            real = code > 0
            code = code + 22
            dx = jnp.where(code >= 200, 2, jnp.where(code >= 100, 1, 0))
            rem = code - dx * 100
            bit = rem - 5 * ((rem * 205) >> 11) - 2
            value = jnp.where(real, jnp.left_shift(1, jnp.where(real, bit, 0)), 0).astype(f32)
            for k in range(3):
                total = jnp.sum(jnp.where(dx == k, value, 0.0), axis=1, keepdims=True)
                total = jnp.concatenate([total, jnp.zeros((ROWS - EDGE, 1), f32)], axis=0)
                spread[k] = spread[k] + jnp.where(lane == y * WIDE + k * EDGE + z, total, 0.0)
    bits = [s.astype(jnp.int32) for s in spread]
    moved = {}

    def flag_tile(n):
        out = jnp.zeros((ROWS, LANES), jnp.int32)
        for d, (c, m) in FLAGS.items():
            if m == n:
                key = (d[0], c)
                if key not in moved:
                    moved[key] = roll(bits[d[0]], (c - d[0]) * EDGE)
                out = out | (lax.shift_right_logical(moved[key], 5 * (d[1] + 2) + d[2]) & 1)
        return out.astype(f32)

    send0[0] = jit
    send0[1] = x
    send0[2] = pol0 + flag_tile(FLAG_TILES)
    for n in range(FLAG_TILES):
        send0[3 + n] = flag_tile(n)
    own = 4
    recv0[own] = send0[...]

    real = pl.ds(0, EDGE)

    def halo_start(index, src, get_dst):
        for oy in (-1, 1, 0):
            for oz in (-1, 1, 0):
                for ox in (1, 0):
                    if (ox, oy, oz) == (0, 0, 0):
                        continue
                    back = ox * 9 + (1 - oy) * 3 + 1 - oz
                    pltpu.make_async_remote_copy(
                        src_ref=src, dst_ref=get_dst(back),
                        send_sem=halo_send.at[index], recv_sem=halo_recv.at[index],
                        device_id=at(ox, oy, oz), device_id_type=MESH,
                    ).start()

    def halo_all(index):
        some = pl.ds(0, 17)
        ref = recv0.at[some, :, real] if index == 0 else recv1.at[index - 1, some, real]
        return pltpu.make_async_remote_copy(
            src_ref=ref, dst_ref=ref, send_sem=halo_send.at[index], recv_sem=halo_recv.at[index],
            device_id=at(1, 0, 0), device_id_type=MESH,
        )

    def assemble(get, c, target, fill=0.0):
        full = []
        for h in range(2):
            part = []
            for b in range(3):
                m = [roll(get(h * 9 + b * 3 + k), 108 * b + EDGE * (k - c)) for k in range(3)]
                part.append(jnp.where(zone[b][0], m[0], jnp.where(zone[b][1], m[1], m[2])))
            full.append((
                jnp.where(lane < 108, part[0], part[1]),
                jnp.where(lane < 88, part[1], part[2]),
                jnp.where(lane < 68, part[2], fill),
            ))
        for t in range(3):
            target[t, 2:8, :] = full[0][t][:6]
            target[t, 8:14, :] = full[1][t][:6]
            target[t, 0:2, :] = full[1][t][4:6]
            target[t, 14:16, :] = full[0][t][:2]

    def shifted(v, i):
        dy, dz = SHIFTS[i]
        s = dy * WIDE + dz + (ORIGIN if len(v) == 3 else 0)
        if s == 0:
            return v
        r = [roll(u, -s) for u in v]
        if len(v) == 3:
            return [jnp.where(lane < LANES - s, r[t], r[t + 1]) for t in range(2)]
        if s > 0:
            return [jnp.where(lane < LANES - s, r[0], r[1]), r[1]]
        return [r[0], jnp.where(lane >= -s, r[1], r[0])]

    halves = (pl.ds(0, 8), pl.ds(8, 8))

    def apply(source, target, last):
        tiles = range(3) if source is None else range(2)

        def shift(i):
            for k in range(3):
                for rows in halves:
                    ref = ext.at[k] if source is None else chain.at[source, k]
                    for t, value in enumerate(shifted([ref[t, rows, :] for t in tiles], i)):
                        sh[i, t, k, rows, :] = value

        sides = [(t, rt) for t in range(2) for rt in range(1 if last else 2)]
        acc = {side: [None] * 3 for side in sides}

        def compute(i):
            for j, dx in enumerate(SPAN[i]):
                n = FIRST[i] + j
                for t, rt in sides:
                    v = [sh[i, t, k, pl.ds(dx + 2 + 4 * rt, 8), :] for k in range(3)]
                    u = [coef[t, rt, n, k] for k in range(3)]
                    iso = coef[t, rt, n, 3]
                    dot = u[0] * v[0] + u[1] * v[1] + u[2] * v[2]
                    for k in range(3):
                        term = u[k] * dot - iso * v[k]
                        old = acc[t, rt][k]
                        acc[t, rt][k] = term if old is None else old + term

        ahead = 4
        for i in range(len(SHIFTS) + ahead):
            if i < len(SHIFTS):
                shift(i)
            if i >= ahead:
                compute(i - ahead)
        for t, rt in sides:
            scale = polo[t, pl.ds(2 + 4 * rt, 8), :]
            for k in range(3):
                out = acc[t, rt][k] * scale
                chain[target, k, t, pl.ds(2 + 4 * rt, 8), :] = out
                if not last:
                    if rt == 0:
                        chain[target, k, t, 14:16, :] = out[0:2]
                    else:
                        chain[target, k, t, 0:2, :] = out[6:8]

    def pack(index):
        parts = []
        for k in range(3):
            a = OWN - EDGE * k
            r = [roll(chain[index, k, t, 2:10, :], -a) for t in range(2)]
            parts.append(jnp.where(lane < LANES - a, r[0], r[1]))
        out = jnp.where(zone[0][0], parts[0], jnp.where(zone[0][1], parts[1], parts[2]))
        return jnp.where(packed, out, 0.0)

    pl.semaphore_wait(barrier, len(others))
    halo_start(0, send0.at[:, real], lambda b: recv0.at[b, :, real])
    chain[...] = jnp.zeros_like(chain)
    halo_all(0).wait_recv()

    for k in range(3):
        assemble(lambda b: recv0[b, 0], k, geo.at[k])
        assemble(lambda b: recv0[b, 1], k, ext.at[k])
    assemble(lambda b: recv0[b, 2], 0, geo.at[4], 1.0)
    geo[3] = lax.rsqrt(geo[4])
    flagged = [
        jnp.where(zone[0][0], 0.0, recv0[b, 2]) * float(2 ** FLAG_TILES) for b in range(18)
    ]
    for n in range(FLAG_TILES):
        for b in range(18):
            flagged[b] = flagged[b] + recv0[b, 3 + n] * float(2 ** n)
    for k in range(3):
        assemble(lambda b: flagged[b], k, words.at[k])

    for i in range(len(SHIFTS)):
        for rows in halves:
            for k in range(4):
                for t, value in enumerate(shifted([geo[k, t, rows, :] for t in range(3)], i)):
                    sgeo[i, t, k, rows, :] = value
            for k in range(3):
                for t, value in enumerate(shifted([words[k, t, rows, :] for t in range(3)], i)):
                    sword[i, t, k, rows, :] = value.astype(jnp.int32)
    for half in range(2):
        rows = pl.ds(8 * half, 8)
        r = [roll(geo[4, t, rows, :], -ORIGIN) for t in range(3)]
        for t in range(2):
            polo[t, rows, :] = jnp.where(lane < LANES - ORIGIN, r[t], r[t + 1])

    def geometry(t, carry):
        for rt in range(2):
            base = 2 + 4 * rt
            here = [sgeo[HOME, t, k, pl.ds(base, 8), :] for k in range(4)]
            flags = [sword[HOME, t, k, pl.ds(base, 8), :] for k in range(3)]
            damped = here[3] * thole_damping
            for i, s in enumerate(SHIFTS):
                for j, dx in enumerate(SPAN[i]):
                    n = FIRST[i] + j
                    d = (dx, *s)
                    rows = pl.ds(base + dx, 8)
                    if d > (0, 0, 0):
                        c, m = FLAGS[d]
                        word = flags[c]
                    else:
                        c, m = FLAGS[tuple(-v for v in d)]
                        word = sword[i, t, c, rows, :]
                    present = (word & (1 << m)) != 0
                    sep = [sgeo[i, t, k, rows, :] - here[k] for k in range(3)]
                    sep = [v + e * site_spacing if e else v for v, e in zip(sep, d)]
                    sq = sep[0] * sep[0] + sep[1] * sep[1] + sep[2] * sep[2]
                    inv = lax.rsqrt(sq)
                    damp = (damped * sgeo[i, t, 3, rows, :]) * (sq * (sq * inv))
                    fall = jnp.exp(-damp)
                    inv2 = inv * inv
                    inv3 = inv2 * inv
                    iso = jnp.where(present, (1.0 - fall) * inv3, 0.0)
                    rad = (1.0 - (1.0 + damp) * fall) * (3.0 * inv3 * inv2)
                    root = jnp.where(present, rad * lax.rsqrt(rad), 0.0)
                    for k in range(3):
                        coef[t, rt, n, k] = root * sep[k]
                    coef[t, rt, n, 3] = iso
        return carry

    lax.fori_loop(0, 2, geometry, 0)

    def dots_start(index, vectors, number):
        line = jnp.zeros((1, LANES), f32)
        for m in range(number):
            value = weight * vectors[m // 2] * vectors[(m + 1) // 2]
            value = jnp.sum(jnp.sum(value, axis=0, keepdims=True), axis=1, keepdims=True)
            line = jnp.where(pick == m, value, line)
        dot_src[index] = line
        dot_dst[index, rank] = line
        for o in others:
            pltpu.make_async_remote_copy(
                src_ref=dot_src.at[index], dst_ref=dot_dst.at[index, rank],
                send_sem=dot_send.at[index], recv_sem=dot_recv.at[index],
                device_id=at(*o), device_id_type=MESH,
            ).start()

    def dots_all(index):
        some = dot_dst.at[index, pl.ds(0, count - 1)]
        return pltpu.make_async_remote_copy(
            src_ref=some, dst_ref=some, send_sem=dot_send.at[index], recv_sem=dot_recv.at[index],
            device_id=at(1, 0, 0), device_id_type=MESH,
        )

    def dots_finish(index, number):
        dots_all(index).wait_recv()
        line = jnp.sum(dot_dst[index, :, 0, :], axis=0, keepdims=True)
        return [
            jnp.broadcast_to(jnp.sum(jnp.where(pick == m, line, 0.0), axis=1, keepdims=True), (ROWS, LANES))
            for m in range(number)
        ]

    def scalars(moments, history, steps):
        number = 2 * steps
        before = [0.0] * number
        if history:
            _, _, mu1, eta1, inv1, _ = history[-1]
            _, _, mu2, eta2, inv2, _ = history[-2]
            before[1] = moments[0] * inv1
            before[2] = moments[1] * inv1 + mu1 * before[1]
            older2 = before[1] * inv2
            before[3] = moments[2] * inv1 + mu1 * before[2] + eta1 * older2
            older3 = before[2] * inv2 + mu2 * older2
            before[4] = moments[3] * inv1 + mu1 * before[3] + eta1 * older3
        now, lead, seen = list(moments), None, 0.0
        out = []
        known = list(history)
        for i in range(steps):
            gamma = now[i] if lead is None else lead * now[i]
            if known:
                eta = gamma * known[-1][4] / known[-1][5]
                beta = eta * known[-1][0]
            else:
                eta = beta = jnp.zeros((ROWS, LANES), f32)
            ratio = now[i + 1] / now[i]
            mu = ratio - seen
            seen = ratio
            inv = 1.0 - mu - eta
            alpha = 1.0 / inv
            later = [0.0] * number
            for m in range(i + 1, number - 1 - i):
                later[m] = alpha * (now[m + 1] - mu * now[m] - eta * before[m])
            before, now = now, later
            lead = alpha if lead is None else lead * alpha
            out.append((alpha, beta, mu, eta, inv, gamma))
            known.append(out[-1])
        return out

    known = []
    table = [[]]

    def lanczos(vectors):
        i = len(table) - 1
        alpha, _, mu, eta, _, _ = known[i]
        now = table[i]
        table.append([
            alpha * (now[m + 1] - mu * now[m] - (eta * table[i - 1][m] if i else 0.0))
            for m in range(vectors)
        ])

    def chain_of_three():
        out = []
        for k in range(3):
            apply(None if k == 0 else k - 1, k, k == 2)
            out.append(pack(k))
        return out

    def share(index, value):
        send1[index] = value
        recv1[index, own] = value
        halo_start(1 + index, send1.at[index, real], lambda b: recv1.at[index, b, real])

    def receive(index):
        halo_all(1 + index).wait_recv()
        for k in range(3):
            assemble(lambda b: recv1[index, b], k, ext.at[k])

    table[0] += chain_of_three()
    share(0, table[0][2])
    dots_start(0, table[0], 4)
    receive(0)
    table[0] += chain_of_three()
    known += scalars(dots_finish(0, 4), known, 2)
    lanczos(5)
    lanczos(4)
    share(1, table[2][3])
    dots_start(1, table[2], 6)
    receive(1)
    table[2] += chain_of_three()
    known += scalars(dots_finish(1, 6), known, 3)
    table[1].append(table[2][4] * known[1][4] + known[1][2] * table[1][4] + known[1][3] * table[0][4])
    for vectors in (6, 5, 4):
        lanczos(vectors)
    dots_start(2, table[5], 6)
    known += scalars(dots_finish(2, 6), known, 3)
    for vectors in (3, 2, 1):
        lanczos(vectors)

    line = jnp.zeros((1, LANES), f32)
    p = None
    for i, (alpha, beta, *_) in enumerate(known):
        p = table[i][0] if p is None else table[i][0] + beta * p
        x = x + alpha * p
        line = jnp.where(pick == i, alpha[0:1], line)
    residual = table[ITERS][0] * weight
    out_ref[0] = x
    out_ref[1] = residual
    out_ref[2, 0:1, :] = line

    for index in range(3):
        halo_all(index).wait_send()
        dots_all(index).wait_send()


def unpack(in_ref, x_out, r_out, len_out):
    for k, ref in enumerate((x_out, r_out)):
        value = in_ref[k]
        for y in range(EDGE):
            for c in range(3):
                ref[:, y, c, :] = roll(value, -(y * WIDE + c * EDGE))[:EDGE, :EDGE]
    len_out[...] = in_ref[2, 0:1, :ITERS]


def solution(mesh):
    sizes = tuple(mesh.shape[a] for a in ("gx", "gy", "gz"))
    assert sizes[0] == 2
    count = sizes[0] * sizes[1] * sizes[2]

    def local(permanent_field, polar, jitter, neighbors):
        assert polar.shape == (EDGE, EDGE, EDGE)
        vmem = pl.BlockSpec(memory_space=pltpu.VMEM)
        shape = jax.ShapeDtypeStruct((EDGE, EDGE, 3, EDGE), f32)
        wide, near = (3, 16, LANES), (2, 16, LANES)
        shifts = len(SHIFTS)
        anywhere = pl.BlockSpec(memory_space=pl.ANY)
        packed = pl.pallas_call(
            functools.partial(kernel, sizes),
            out_shape=pltpu.VMEM((3, ROWS, LANES), f32),
            in_specs=[anywhere] * 4,
            out_specs=vmem,
            scratch_shapes=[
                pltpu.VMEM((EDGE, EDGE, 3, EDGE), f32),
                pltpu.VMEM((EDGE, EDGE, EDGE), f32),
                pltpu.VMEM((EDGE, EDGE, 3, EDGE), f32),
                pltpu.VMEM(neighbors.shape, jnp.int32),
                pltpu.VMEM((3, *wide), f32),
                pltpu.VMEM((shifts, 2, 3, 16, LANES), f32),
                pltpu.VMEM((5, *wide), f32),
                pltpu.VMEM((3, *wide), f32),
                pltpu.VMEM((shifts, 2, 4, 16, LANES), f32),
                pltpu.VMEM((shifts, 2, 3, 16, LANES), jnp.int32),
                pltpu.VMEM(near, f32),
                pltpu.VMEM((2, 2, len(STENCIL), 4, ROWS, LANES), f32),
                pltpu.VMEM((3, 3, *near), f32),
                pltpu.VMEM((TILES, ROWS, LANES), f32),
                pltpu.VMEM((18, TILES, ROWS, LANES), f32),
                pltpu.VMEM((2, ROWS, LANES), f32),
                pltpu.VMEM((2, 18, ROWS, LANES), f32),
                pltpu.VMEM((3, 1, LANES), f32),
                pltpu.VMEM((3, count, 1, LANES), f32),
                pltpu.SemaphoreType.DMA((3,)),
                pltpu.SemaphoreType.DMA((3,)),
                pltpu.SemaphoreType.DMA((3,)),
                pltpu.SemaphoreType.DMA((3,)),
                pltpu.SemaphoreType.DMA((4,)),
            ],
            compiler_params=pltpu.CompilerParams(collective_id=0, has_side_effects=True),
        )(
            jnp.moveaxis(permanent_field, -1, 2),
            polar,
            jnp.moveaxis(jitter, -1, 2),
            neighbors,
        )
        x, r, steps = pl.pallas_call(
            unpack,
            out_shape=(shape, shape, jax.ShapeDtypeStruct((1, ITERS), f32)),
            in_specs=[vmem],
            out_specs=(vmem, vmem, vmem),
        )(pltpu.with_memory_space_constraint(packed, pltpu.VMEM))
        return jnp.moveaxis(x, 2, -1), jnp.moveaxis(r, 2, -1), steps.reshape(ITERS)

    return jax.shard_map(
        local,
        mesh=mesh,
        in_specs=(
            P("gx", "gy", "gz", None),
            P("gx", "gy", "gz"),
            P("gx", "gy", "gz", None),
            P("gx", "gy", "gz", None),
        ),
        out_specs=(P("gx", "gy", "gz", None), P("gx", "gy", "gz", None), P()),
        check_vma=False,
    )
```

```python
import functools

import jax
import jax.numpy as jnp
from jax import lax
from jax.experimental import pallas as pl
from jax.experimental.pallas import tpu as pltpu
from jax.sharding import PartitionSpec as P

ITERS = 8
MESH = pl.DeviceIdType.MESH
thole_damping = 0.39
site_spacing = 3.5
ROWS, LANES = 8, 128
EDGE = 6
WIDE = 3 * EDGE
ORIGIN = 2 * WIDE + 2
OWN = EDGE * WIDE + EDGE - ORIGIN
f32 = jnp.float32

STENCIL = [
    (a, b, c)
    for a in range(-2, 3)
    for b in range(-2, 3)
    for c in range(-2, 3)
    if 1 <= a * a + b * b + c * c <= 5
]
SHIFTS = sorted({(b, c) for a, b, c in STENCIL})
SPAN = [[d[0] for d in STENCIL if d[1:] == s] for s in SHIFTS]
FIRST = [sum(len(v) for v in SPAN[:i]) for i in range(len(SHIFTS))]
HOME = SHIFTS.index((0, 0))
FORWARD = [d for d in STENCIL if d > (0, 0, 0)]


def flag_places():
    room = {0: 9, 1: 10, 2: 10}
    used = {0: 0, 1: 0, 2: 0}
    places = {}
    for d in FORWARD:
        c = d[0] if used[d[0]] < room[d[0]] else 2
        if d[0] != 2 and used[d[0]] >= room[d[0]]:
            c = 2
        places[d] = (c, used[c])
        used[c] += 1
    assert used[2] <= room[2]
    return places


FLAGS = flag_places()
FLAG_TILES = 9
TILES = 3
GREET_Y = (0, 1, 3)
GREET_Z = (0, 1, 4, 7, 9, 12, 15)


def roll(value, shift):
    shift = shift % LANES
    return value if shift == 0 else pltpu.roll(value, shift, axis=1)


def kernel(
    sizes,
    field_in, pol_in, jit_in, nb_in, out_ref,
    field_ref, pol_ref, jit_ref, nb_ref,
    ext, sh, geo, words, sgeo, sword, polo, coef, chain,
    send0, recv0, sendf, recvf, send1, recv1, dot_src, dot_dst,
    halo_send, halo_recv, dot_send, dot_recv, in_sems,
):
    nx, ny, nz = sizes
    count = nx * ny * nz
    gx, gy, gz = lax.axis_index("gx"), lax.axis_index("gy"), lax.axis_index("gz")
    rank = (gx * ny + gy) * nz + gz

    def at(ox, oy, oz):
        return (lax.rem(gx + ox + nx, nx), lax.rem(gy + oy + ny, ny), lax.rem(gz + oz + nz, nz))

    others = [
        (a, b, c) for a in range(nx) for b in range(ny) for c in range(nz) if (a, b, c) != (0, 0, 0)
    ]
    others.sort(key=lambda o: -(min(o[0], nx - o[0]) + 2 * min(o[1], ny - o[1]) + 2 * min(o[2], nz - o[2])))

    barrier = pltpu.get_barrier_semaphore()
    loads = [
        pltpu.make_async_copy(source, target, in_sems.at[k])
        for k, (source, target) in enumerate((
            (nb_in, nb_ref), (field_in, field_ref), (pol_in, pol_ref), (jit_in, jit_ref),
        ))
    ]
    for load in loads:
        load.start()
    greeted = [o for o in others if o[1] in GREET_Y and o[2] in GREET_Z]
    for o in greeted:
        pl.semaphore_signal(barrier, inc=1, device_id=at(*o), device_id_type=MESH)
    lane = lax.broadcasted_iota(jnp.int32, (ROWS, LANES), 1)
    row = lax.broadcasted_iota(jnp.int32, (ROWS, LANES), 0)
    pick = lax.broadcasted_iota(jnp.int32, (1, LANES), 1)

    def third(b):
        position = lax.rem(lane - 108 * b + 2 * LANES * 2, LANES)
        within = position - (position // WIDE) * WIDE
        return within < EDGE, within < 2 * EDGE

    zone = [third(b) for b in range(3)]
    packed = (row < EDGE) & (lane < EDGE * WIDE)

    def gather3(ref, comps):
        out = jnp.zeros((ROWS, LANES), f32)
        for y in range(EDGE):
            for c in range(comps):
                part = ref[:, y, c, :] if comps == 3 else ref[:, y, :]
                part = jnp.concatenate([part, jnp.zeros((EDGE, LANES - EDGE), f32)], axis=1)
                part = jnp.concatenate([part, jnp.zeros((ROWS - EDGE, LANES), f32)], axis=0)
                out = out + roll(part, y * WIDE + c * EDGE)
        return out

    for load in loads:
        load.wait()
    field, jit = gather3(field_ref, 3), gather3(jit_ref, 3) * site_spacing
    pol0 = gather3(pol_ref, 1)
    polp = pol0 + roll(pol0, EDGE) + roll(pol0, 2 * EDGE)
    weight = jnp.where(packed, 1.0 / jnp.where(packed, polp, 1.0), 0.0)
    x = polp * field

    slots = nb_ref.shape[3]
    plane = lax.broadcasted_iota(jnp.int32, (EDGE, slots), 0) * 100
    spread = [jnp.zeros((ROWS, LANES), f32) for _ in range(3)]
    for y in range(EDGE):
        for z in range(EDGE):
            entry = nb_ref[:, y, z, :]
            code = entry - plane - (222 + 10 * y + z)
            real = code > 0
            code = code + 22
            dx = jnp.where(code >= 200, 2, jnp.where(code >= 100, 1, 0))
            rem = code - dx * 100
            bit = rem - 5 * ((rem * 205) >> 11) - 2
            value = jnp.where(real, jnp.left_shift(1, jnp.where(real, bit, 0)), 0).astype(f32)
            for k in range(3):
                total = jnp.sum(jnp.where(dx == k, value, 0.0), axis=1, keepdims=True)
                total = jnp.concatenate([total, jnp.zeros((ROWS - EDGE, 1), f32)], axis=0)
                spread[k] = spread[k] + jnp.where(lane == y * WIDE + k * EDGE + z, total, 0.0)
    bits = [s.astype(jnp.int32) for s in spread]
    moved = {}

    def flag_tile(n):
        out = jnp.zeros((ROWS, LANES), jnp.int32)
        for d, (c, m) in FLAGS.items():
            if m == n:
                key = (d[0], c)
                if key not in moved:
                    moved[key] = roll(bits[d[0]], (c - d[0]) * EDGE)
                out = out | (lax.shift_right_logical(moved[key], 5 * (d[1] + 2) + d[2]) & 1)
        return out.astype(f32)

    send0[0] = jit
    send0[1] = x
    send0[2] = pol0 + flag_tile(FLAG_TILES)
    for n in range(FLAG_TILES):
        sendf[n] = flag_tile(n)
    own = 4
    recv0[own] = send0[...]
    recvf[own] = sendf[...]

    real = pl.ds(0, EDGE)

    def halo_start(index, src, get_dst):
        for oy in (-1, 1, 0):
            for oz in (-1, 1, 0):
                for ox in (1, 0):
                    if (ox, oy, oz) == (0, 0, 0):
                        continue
                    back = ox * 9 + (1 - oy) * 3 + 1 - oz
                    pltpu.make_async_remote_copy(
                        src_ref=src, dst_ref=get_dst(back),
                        send_sem=halo_send.at[index], recv_sem=halo_recv.at[index],
                        device_id=at(ox, oy, oz), device_id_type=MESH,
                    ).start()

    def halo_all(index):
        some = pl.ds(0, 17)
        ref = {
            0: recv0.at[some, :, real], 3: recvf.at[some, :, real],
            1: recv1.at[0, some, real], 2: recv1.at[1, some, real],
        }[index]
        return pltpu.make_async_remote_copy(
            src_ref=ref, dst_ref=ref, send_sem=halo_send.at[index], recv_sem=halo_recv.at[index],
            device_id=at(1, 0, 0), device_id_type=MESH,
        )

    def assemble(get, c, target, fill=0.0):
        full = []
        for h in range(2):
            part = []
            for b in range(3):
                m = [roll(get(h * 9 + b * 3 + k), 108 * b + EDGE * (k - c)) for k in range(3)]
                part.append(jnp.where(zone[b][0], m[0], jnp.where(zone[b][1], m[1], m[2])))
            full.append((
                jnp.where(lane < 108, part[0], part[1]),
                jnp.where(lane < 88, part[1], part[2]),
                jnp.where(lane < 68, part[2], fill),
            ))
        for t in range(3):
            target[t, 2:8, :] = full[0][t][:6]
            target[t, 8:14, :] = full[1][t][:6]
            target[t, 0:2, :] = full[1][t][4:6]
            target[t, 14:16, :] = full[0][t][:2]

    def shifted(v, i):
        dy, dz = SHIFTS[i]
        s = dy * WIDE + dz + (ORIGIN if len(v) == 3 else 0)
        if s == 0:
            return v
        r = [roll(u, -s) for u in v]
        if len(v) == 3:
            return [jnp.where(lane < LANES - s, r[t], r[t + 1]) for t in range(2)]
        if s > 0:
            return [jnp.where(lane < LANES - s, r[0], r[1]), r[1]]
        return [r[0], jnp.where(lane >= -s, r[1], r[0])]

    halves = (pl.ds(0, 8), pl.ds(8, 8))

    def in_order(shift, compute, ahead=4):
        order = [HOME] + [i for i in range(len(SHIFTS)) if i != HOME]
        for place in range(len(order) + ahead):
            if place < len(order):
                shift(order[place])
            if place >= ahead:
                compute(order[place - ahead])

    def apply(source, target, last, masked=False):
        tiles = range(3) if source is None else range(2)

        def shift(i):
            for k in range(3):
                for rows in halves:
                    ref = ext.at[k] if source is None else chain.at[source, k]
                    for t, value in enumerate(shifted([ref[t, rows, :] for t in tiles], i)):
                        sh[i, t, k, rows, :] = value
                    if masked:
                        for t, value in enumerate(shifted([words[k, t, rows, :] for t in tiles], i)):
                            sword[i, t, k, rows, :] = value

        def present(i, dx, t, rt):
            d = (dx, *SHIFTS[i])
            if d > (0, 0, 0):
                c, m = FLAGS[d]
                word = sword[HOME, t, c, pl.ds(2 + 4 * rt, 8), :]
            else:
                c, m = FLAGS[tuple(-v for v in d)]
                word = sword[i, t, c, pl.ds(2 + 4 * rt + dx, 8), :]
            return (word & (1 << m)) != 0

        sides = [(t, rt) for t in range(2) for rt in range(1 if last else 2)]
        acc = {side: [None] * 3 for side in sides}

        def compute(i):
            for j, dx in enumerate(SPAN[i]):
                n = FIRST[i] + j
                for t, rt in sides:
                    v = [sh[i, t, k, pl.ds(dx + 2 + 4 * rt, 8), :] for k in range(3)]
                    u = [coef[t, rt, n, k] for k in range(3)]
                    iso = coef[t, rt, n, 3]
                    if masked:
                        there = present(i, dx, t, rt)
                        u = [jnp.where(there, value, 0.0) for value in u]
                        iso = jnp.where(there, iso, 0.0)
                        for k, value in enumerate((*u, iso)):
                            coef[t, rt, n, k] = value
                    dot = u[0] * v[0] + u[1] * v[1] + u[2] * v[2]
                    for k in range(3):
                        term = u[k] * dot - iso * v[k]
                        old = acc[t, rt][k]
                        acc[t, rt][k] = term if old is None else old + term

        in_order(shift, compute)
        for t, rt in sides:
            scale = polo[t, pl.ds(2 + 4 * rt, 8), :]
            for k in range(3):
                out = acc[t, rt][k] * scale
                chain[target, k, t, pl.ds(2 + 4 * rt, 8), :] = out
                if not last:
                    if rt == 0:
                        chain[target, k, t, 14:16, :] = out[0:2]
                    else:
                        chain[target, k, t, 0:2, :] = out[6:8]

    def pack(index):
        parts = []
        for k in range(3):
            a = OWN - EDGE * k
            r = [roll(chain[index, k, t, 2:10, :], -a) for t in range(2)]
            parts.append(jnp.where(lane < LANES - a, r[0], r[1]))
        out = jnp.where(zone[0][0], parts[0], jnp.where(zone[0][1], parts[1], parts[2]))
        return jnp.where(packed, out, 0.0)

    pl.semaphore_wait(barrier, len(greeted))
    halo_start(0, send0.at[:, real], lambda b: recv0.at[b, :, real])
    halo_start(3, sendf.at[:, real], lambda b: recvf.at[b, :, real])
    chain[...] = jnp.zeros_like(chain)
    halo_all(0).wait_recv()

    for k in range(3):
        assemble(lambda b: recv0[b, 0], k, geo.at[k])
        assemble(lambda b: recv0[b, 1], k, ext.at[k])
    assemble(lambda b: recv0[b, 2], 0, geo.at[4], 1.0)
    geo[3] = lax.rsqrt(geo[4])
    for half in range(2):
        rows = pl.ds(8 * half, 8)
        r = [roll(geo[4, t, rows, :], -ORIGIN) for t in range(3)]
        for t in range(2):
            polo[t, rows, :] = jnp.where(lane < LANES - ORIGIN, r[t], r[t + 1])

    def geometry(t, carry):
        def shift(i):
            a = ORIGIN + SHIFTS[i][0] * WIDE + SHIFTS[i][1]
            for rows in halves:
                for k in range(4):
                    pair = [roll(geo[k, t + u, rows, :], -a) for u in range(2)]
                    sgeo[i, t, k, rows, :] = jnp.where(lane < LANES - a, pair[0], pair[1])

        def compute(i):
            for rt in range(2):
                base = 2 + 4 * rt
                for j, dx in enumerate(SPAN[i]):
                    n = FIRST[i] + j
                    d = (dx, *SHIFTS[i])
                    rows = pl.ds(base + dx, 8)
                    sep = [sgeo[i, t, k, rows, :] - sgeo[HOME, t, k, pl.ds(base, 8), :] for k in range(3)]
                    sep = [v + e * site_spacing if e else v for v, e in zip(sep, d)]
                    sq = sep[0] * sep[0] + sep[1] * sep[1] + sep[2] * sep[2]
                    inv = lax.rsqrt(sq)
                    roots = sgeo[HOME, t, 3, pl.ds(base, 8), :] * sgeo[i, t, 3, rows, :]
                    damp = (thole_damping * roots) * (sq * (sq * inv))
                    fall = jnp.exp(-damp)
                    inv2 = inv * inv
                    inv3 = inv2 * inv
                    rad = (1.0 - (1.0 + damp) * fall) * (3.0 * inv3 * inv2)
                    root = rad * lax.rsqrt(rad)
                    for k in range(3):
                        coef[t, rt, n, k] = root * sep[k]
                    coef[t, rt, n, 3] = (1.0 - fall) * inv3

        in_order(shift, compute)
        return carry

    lax.fori_loop(0, 2, geometry, 0)

    halo_all(3).wait_recv()
    flagged = []
    for b in range(18):
        total = jnp.where(zone[0][0], 0.0, recv0[b, 2]) * float(2 ** FLAG_TILES)
        for n in range(FLAG_TILES):
            total = total + recvf[b, n] * float(2 ** n)
        flagged.append(total.astype(jnp.int32))
    for k in range(3):
        assemble(lambda b: flagged[b], k, words.at[k], 0)

    def dots_start(index, vectors, number):
        line = jnp.zeros((1, LANES), f32)
        for m in range(number):
            value = weight * vectors[m // 2] * vectors[(m + 1) // 2]
            value = jnp.sum(jnp.sum(value, axis=0, keepdims=True), axis=1, keepdims=True)
            line = jnp.where(pick == m, value, line)
        dot_src[index] = line
        dot_dst[index, rank] = line
        for o in others:
            pltpu.make_async_remote_copy(
                src_ref=dot_src.at[index], dst_ref=dot_dst.at[index, rank],
                send_sem=dot_send.at[index], recv_sem=dot_recv.at[index],
                device_id=at(*o), device_id_type=MESH,
            ).start()

    def dots_all(index):
        some = dot_dst.at[index, pl.ds(0, count - 1)]
        return pltpu.make_async_remote_copy(
            src_ref=some, dst_ref=some, send_sem=dot_send.at[index], recv_sem=dot_recv.at[index],
            device_id=at(1, 0, 0), device_id_type=MESH,
        )

    def dots_finish(index, number):
        dots_all(index).wait_recv()
        line = jnp.sum(dot_dst[index, :, 0, :], axis=0, keepdims=True)
        return [
            jnp.broadcast_to(jnp.sum(jnp.where(pick == m, line, 0.0), axis=1, keepdims=True), (ROWS, LANES))
            for m in range(number)
        ]

    def scalars(moments, history, steps):
        number = 2 * steps
        before = [0.0] * number
        if history:
            _, _, mu1, eta1, inv1, _ = history[-1]
            _, _, mu2, eta2, inv2, _ = history[-2]
            before[1] = moments[0] * inv1
            before[2] = moments[1] * inv1 + mu1 * before[1]
            older2 = before[1] * inv2
            before[3] = moments[2] * inv1 + mu1 * before[2] + eta1 * older2
            older3 = before[2] * inv2 + mu2 * older2
            before[4] = moments[3] * inv1 + mu1 * before[3] + eta1 * older3
        now, lead, seen = list(moments), None, 0.0
        out = []
        known = list(history)
        for i in range(steps):
            gamma = now[i] if lead is None else lead * now[i]
            if known:
                eta = gamma * known[-1][4] / known[-1][5]
                beta = eta * known[-1][0]
            else:
                eta = beta = jnp.zeros((ROWS, LANES), f32)
            ratio = now[i + 1] / now[i]
            mu = ratio - seen
            seen = ratio
            inv = 1.0 - mu - eta
            alpha = 1.0 / inv
            later = [0.0] * number
            for m in range(i + 1, number - 1 - i):
                later[m] = alpha * (now[m + 1] - mu * now[m] - eta * before[m])
            before, now = now, later
            lead = alpha if lead is None else lead * alpha
            out.append((alpha, beta, mu, eta, inv, gamma))
            known.append(out[-1])
        return out

    known = []
    table = [[]]

    def lanczos(vectors):
        i = len(table) - 1
        alpha, _, mu, eta, _, _ = known[i]
        now = table[i]
        table.append([
            alpha * (now[m + 1] - mu * now[m] - (eta * table[i - 1][m] if i else 0.0))
            for m in range(vectors)
        ])

    def chain_of_three(first=False):
        out = []
        for k in range(3):
            apply(None if k == 0 else k - 1, k, k == 2, first and k == 0)
            out.append(pack(k))
        return out

    def share(index, value):
        send1[index] = value
        recv1[index, own] = value
        halo_start(1 + index, send1.at[index, real], lambda b: recv1.at[index, b, real])

    def receive(index):
        halo_all(1 + index).wait_recv()
        for k in range(3):
            assemble(lambda b: recv1[index, b], k, ext.at[k])

    table[0] += chain_of_three(True)
    share(0, table[0][2])
    dots_start(0, table[0], 4)
    receive(0)
    table[0] += chain_of_three()
    known += scalars(dots_finish(0, 4), known, 2)
    lanczos(5)
    lanczos(4)
    share(1, table[2][3])
    dots_start(1, table[2], 6)
    receive(1)
    table[2] += chain_of_three()
    known += scalars(dots_finish(1, 6), known, 3)
    table[1].append(table[2][4] * known[1][4] + known[1][2] * table[1][4] + known[1][3] * table[0][4])
    for vectors in (6, 5, 4):
        lanczos(vectors)
    dots_start(2, table[5], 6)
    known += scalars(dots_finish(2, 6), known, 3)
    for vectors in (3, 2, 1):
        lanczos(vectors)

    line = jnp.zeros((1, LANES), f32)
    p = None
    for i, (alpha, beta, *_) in enumerate(known):
        p = table[i][0] if p is None else table[i][0] + beta * p
        x = x + alpha * p
        line = jnp.where(pick == i, alpha[0:1], line)
    residual = table[ITERS][0] * weight
    out_ref[0] = x
    out_ref[1] = residual
    out_ref[2, 0:1, :] = line

    for index in range(4):
        halo_all(index).wait_send()
    for index in range(3):
        dots_all(index).wait_send()


def unpack(in_ref, x_out, r_out, len_out):
    for k, ref in enumerate((x_out, r_out)):
        value = in_ref[k]
        for y in range(EDGE):
            for c in range(3):
                ref[:, y, c, :] = roll(value, -(y * WIDE + c * EDGE))[:EDGE, :EDGE]
    len_out[...] = in_ref[2, 0:1, :ITERS]


def solution(mesh):
    sizes = tuple(mesh.shape[a] for a in ("gx", "gy", "gz"))
    assert sizes[0] == 2
    count = sizes[0] * sizes[1] * sizes[2]

    def local(permanent_field, polar, jitter, neighbors):
        assert polar.shape == (EDGE, EDGE, EDGE)
        vmem = pl.BlockSpec(memory_space=pltpu.VMEM)
        shape = jax.ShapeDtypeStruct((EDGE, EDGE, 3, EDGE), f32)
        wide, near = (3, 16, LANES), (2, 16, LANES)
        shifts = len(SHIFTS)
        anywhere = pl.BlockSpec(memory_space=pl.ANY)
        packed = pl.pallas_call(
            functools.partial(kernel, sizes),
            out_shape=pltpu.VMEM((3, ROWS, LANES), f32),
            in_specs=[anywhere] * 4,
            out_specs=vmem,
            scratch_shapes=[
                pltpu.VMEM((EDGE, EDGE, 3, EDGE), f32),
                pltpu.VMEM((EDGE, EDGE, EDGE), f32),
                pltpu.VMEM((EDGE, EDGE, 3, EDGE), f32),
                pltpu.VMEM(neighbors.shape, jnp.int32),
                pltpu.VMEM((3, *wide), f32),
                pltpu.VMEM((shifts, 2, 3, 16, LANES), f32),
                pltpu.VMEM((5, *wide), f32),
                pltpu.VMEM((3, *wide), jnp.int32),
                pltpu.VMEM((shifts, 2, 4, 16, LANES), f32),
                pltpu.VMEM((shifts, 2, 3, 16, LANES), jnp.int32),
                pltpu.VMEM(near, f32),
                pltpu.VMEM((2, 2, len(STENCIL), 4, ROWS, LANES), f32),
                pltpu.VMEM((3, 3, *near), f32),
                pltpu.VMEM((TILES, ROWS, LANES), f32),
                pltpu.VMEM((18, TILES, ROWS, LANES), f32),
                pltpu.VMEM((FLAG_TILES, ROWS, LANES), f32),
                pltpu.VMEM((18, FLAG_TILES, ROWS, LANES), f32),
                pltpu.VMEM((2, ROWS, LANES), f32),
                pltpu.VMEM((2, 18, ROWS, LANES), f32),
                pltpu.VMEM((3, 1, LANES), f32),
                pltpu.VMEM((3, count, 1, LANES), f32),
                pltpu.SemaphoreType.DMA((4,)),
                pltpu.SemaphoreType.DMA((4,)),
                pltpu.SemaphoreType.DMA((3,)),
                pltpu.SemaphoreType.DMA((3,)),
                pltpu.SemaphoreType.DMA((4,)),
            ],
            compiler_params=pltpu.CompilerParams(collective_id=0, has_side_effects=True),
        )(
            jnp.moveaxis(permanent_field, -1, 2),
            polar,
            jnp.moveaxis(jitter, -1, 2),
            neighbors,
        )
        x, r, steps = pl.pallas_call(
            unpack,
            out_shape=(shape, shape, jax.ShapeDtypeStruct((1, ITERS), f32)),
            in_specs=[vmem],
            out_specs=(vmem, vmem, vmem),
        )(pltpu.with_memory_space_constraint(packed, pltpu.VMEM))
        return jnp.moveaxis(x, 2, -1), jnp.moveaxis(r, 2, -1), steps.reshape(ITERS)

    return jax.shard_map(
        local,
        mesh=mesh,
        in_specs=(
            P("gx", "gy", "gz", None),
            P("gx", "gy", "gz"),
            P("gx", "gy", "gz", None),
            P("gx", "gy", "gz", None),
        ),
        out_specs=(P("gx", "gy", "gz", None), P("gx", "gy", "gz", None), P()),
        check_vma=False,
    )
```

```python
import functools

import jax
import jax.numpy as jnp
from jax import lax
from jax.experimental import pallas as pl
from jax.experimental.pallas import tpu as pltpu
from jax.sharding import PartitionSpec as P

ITERS = 8
MESH = pl.DeviceIdType.MESH
thole_damping = 0.39
site_spacing = 3.5
ROWS, LANES = 8, 128
EDGE = 6
WIDE = 3 * EDGE
ORIGIN = 2 * WIDE + 2
OWN = EDGE * WIDE + EDGE - ORIGIN
f32 = jnp.float32

STENCIL = [
    (a, b, c)
    for a in range(-2, 3)
    for b in range(-2, 3)
    for c in range(-2, 3)
    if 1 <= a * a + b * b + c * c <= 5
]
SHIFTS = sorted({(b, c) for a, b, c in STENCIL})
SPAN = [[d[0] for d in STENCIL if d[1:] == s] for s in SHIFTS]
FIRST = [sum(len(v) for v in SPAN[:i]) for i in range(len(SHIFTS))]
HOME = SHIFTS.index((0, 0))
FORWARD = [d for d in STENCIL if d > (0, 0, 0)]


def flag_places():
    room = {0: 9, 1: 10, 2: 10}
    used = {0: 0, 1: 0, 2: 0}
    places = {}
    for d in FORWARD:
        c = d[0] if used[d[0]] < room[d[0]] else 2
        if d[0] != 2 and used[d[0]] >= room[d[0]]:
            c = 2
        places[d] = (c, used[c])
        used[c] += 1
    assert used[2] <= room[2]
    return places


FLAGS = flag_places()
FLAG_TILES = 9
TILES = 3
GREET_Y = (0, 1, 3)
GREET_Z = (0, 1, 4, 7, 9, 12, 15)


def roll(value, shift):
    shift = shift % LANES
    return value if shift == 0 else pltpu.roll(value, shift, axis=1)


def kernel(
    sizes,
    field_in, pol_in, jit_in, nb_in, out_ref,
    field_ref, pol_ref, jit_ref, nb_ref,
    ext, sh, geo, words, sgeo, sword, polo, coef, chain,
    send0, recv0, sendf, recvf, send1, recv1, dot_src, dot_dst,
    halo_send, halo_recv, dot_send, dot_recv, in_sems,
):
    nx, ny, nz = sizes
    count = nx * ny * nz
    gx, gy, gz = lax.axis_index("gx"), lax.axis_index("gy"), lax.axis_index("gz")
    rank = (gx * ny + gy) * nz + gz

    def at(ox, oy, oz):
        return (lax.rem(gx + ox + nx, nx), lax.rem(gy + oy + ny, ny), lax.rem(gz + oz + nz, nz))

    others = [
        (a, b, c) for a in range(nx) for b in range(ny) for c in range(nz) if (a, b, c) != (0, 0, 0)
    ]

    def hops(o):
        ring = lambda v: min(v % 4, -v % 4)
        along = max(ring(o[2] // 4), ring(o[2] // 4 + 1)) if o[2] % 4 else ring(o[2] // 4)
        return 4 * (ring(o[1]) + ring(o[2] % 4) + along) + o[0]

    others.sort(key=lambda o: -hops(o))

    barrier = pltpu.get_barrier_semaphore()
    loads = [
        pltpu.make_async_copy(source, target, in_sems.at[k])
        for k, (source, target) in enumerate((
            (nb_in, nb_ref), (field_in, field_ref), (pol_in, pol_ref), (jit_in, jit_ref),
        ))
    ]
    for load in loads:
        load.start()
    greeted = [o for o in others if o[1] in GREET_Y and o[2] in GREET_Z]
    for o in greeted:
        pl.semaphore_signal(barrier, inc=1, device_id=at(*o), device_id_type=MESH)
    lane = lax.broadcasted_iota(jnp.int32, (ROWS, LANES), 1)
    row = lax.broadcasted_iota(jnp.int32, (ROWS, LANES), 0)
    pick = lax.broadcasted_iota(jnp.int32, (1, LANES), 1)

    def third(b):
        position = lax.rem(lane - 108 * b + 2 * LANES * 2, LANES)
        within = position - (position // WIDE) * WIDE
        return within < EDGE, within < 2 * EDGE

    zone = [third(b) for b in range(3)]
    packed = (row < EDGE) & (lane < EDGE * WIDE)

    def gather3(ref, comps):
        out = jnp.zeros((ROWS, LANES), f32)
        for y in range(EDGE):
            for c in range(comps):
                part = ref[:, y, c, :] if comps == 3 else ref[:, y, :]
                part = jnp.concatenate([part, jnp.zeros((EDGE, LANES - EDGE), f32)], axis=1)
                part = jnp.concatenate([part, jnp.zeros((ROWS - EDGE, LANES), f32)], axis=0)
                out = out + roll(part, y * WIDE + c * EDGE)
        return out

    for load in loads:
        load.wait()
    field, jit = gather3(field_ref, 3), gather3(jit_ref, 3) * site_spacing
    pol0 = gather3(pol_ref, 1)
    polp = pol0 + roll(pol0, EDGE) + roll(pol0, 2 * EDGE)
    weight = jnp.where(packed, 1.0 / jnp.where(packed, polp, 1.0), 0.0)
    x = polp * field

    slots = nb_ref.shape[3]
    plane = lax.broadcasted_iota(jnp.int32, (EDGE, slots), 0) * 100
    spread = [jnp.zeros((ROWS, LANES), f32) for _ in range(3)]
    for y in range(EDGE):
        for z in range(EDGE):
            entry = nb_ref[:, y, z, :]
            code = entry - plane - (222 + 10 * y + z)
            real = code > 0
            code = code + 22
            dx = jnp.where(code >= 200, 2, jnp.where(code >= 100, 1, 0))
            rem = code - dx * 100
            bit = rem - 5 * ((rem * 205) >> 11) - 2
            value = jnp.where(real, jnp.left_shift(1, jnp.where(real, bit, 0)), 0).astype(f32)
            for k in range(3):
                total = jnp.sum(jnp.where(dx == k, value, 0.0), axis=1, keepdims=True)
                total = jnp.concatenate([total, jnp.zeros((ROWS - EDGE, 1), f32)], axis=0)
                spread[k] = spread[k] + jnp.where(lane == y * WIDE + k * EDGE + z, total, 0.0)
    bits = [s.astype(jnp.int32) for s in spread]
    moved = {}

    def flag_tile(n):
        out = jnp.zeros((ROWS, LANES), jnp.int32)
        for d, (c, m) in FLAGS.items():
            if m == n:
                key = (d[0], c)
                if key not in moved:
                    moved[key] = roll(bits[d[0]], (c - d[0]) * EDGE)
                out = out | (lax.shift_right_logical(moved[key], 5 * (d[1] + 2) + d[2]) & 1)
        return out.astype(f32)

    send0[0] = jit
    send0[1] = x
    send0[2] = pol0 + flag_tile(FLAG_TILES)
    for n in range(FLAG_TILES):
        sendf[n] = flag_tile(n)
    own = 4
    recv0[own] = send0[...]
    recvf[own] = sendf[...]

    real = pl.ds(0, EDGE)

    def halo_start(index, src, get_dst, wanted=lambda o: True):
        for oy in (-1, 1, 0):
            for oz in (-1, 1, 0):
                for ox in (1, 0):
                    if (ox, oy, oz) == (0, 0, 0) or not wanted((ox, oy, oz)):
                        continue
                    back = ox * 9 + (1 - oy) * 3 + 1 - oz
                    pltpu.make_async_remote_copy(
                        src_ref=src, dst_ref=get_dst(back),
                        send_sem=halo_send.at[index], recv_sem=halo_recv.at[index],
                        device_id=at(ox, oy, oz), device_id_type=MESH,
                    ).start()

    def halo_all(index):
        some = pl.ds(0, 17)
        ref = {
            0: recv0.at[some, :, real],
            3: recvf.at[pl.ds(0, 9), :, real], 4: recvf.at[pl.ds(0, 8), :, real],
            1: recv1.at[0, some, real], 2: recv1.at[1, some, real],
        }[index]
        return pltpu.make_async_remote_copy(
            src_ref=ref, dst_ref=ref, send_sem=halo_send.at[index], recv_sem=halo_recv.at[index],
            device_id=at(1, 0, 0), device_id_type=MESH,
        )

    def assemble(get, c, target, fill=0.0):
        full = []
        for h in range(2):
            part = []
            for b in range(3):
                m = [roll(get(h * 9 + b * 3 + k), 108 * b + EDGE * (k - c)) for k in range(3)]
                part.append(jnp.where(zone[b][0], m[0], jnp.where(zone[b][1], m[1], m[2])))
            full.append((
                jnp.where(lane < 108, part[0], part[1]),
                jnp.where(lane < 88, part[1], part[2]),
                jnp.where(lane < 68, part[2], fill),
            ))
        for t in range(3):
            target[t, 2:8, :] = full[0][t][:6]
            target[t, 8:14, :] = full[1][t][:6]
            target[t, 0:2, :] = full[1][t][4:6]
            target[t, 14:16, :] = full[0][t][:2]

    def shifted(v, i):
        dy, dz = SHIFTS[i]
        s = dy * WIDE + dz + (ORIGIN if len(v) == 3 else 0)
        if s == 0:
            return v
        r = [roll(u, -s) for u in v]
        if len(v) == 3:
            return [jnp.where(lane < LANES - s, r[t], r[t + 1]) for t in range(2)]
        if s > 0:
            return [jnp.where(lane < LANES - s, r[0], r[1]), r[1]]
        return [r[0], jnp.where(lane >= -s, r[1], r[0])]

    halves = (pl.ds(0, 8), pl.ds(8, 8))

    def in_order(shift, compute, ahead=4):
        order = [HOME] + [i for i in range(len(SHIFTS)) if i != HOME]
        for place in range(len(order) + ahead):
            if place < len(order):
                shift(order[place])
            if place >= ahead:
                compute(order[place - ahead])

    def apply(source, target, last, masked=False):
        tiles = range(3) if source is None else range(2)
        needed = [
            {FLAGS[tuple(-v for v in (dx, *s))][0] for dx in span if (dx, *s) < (0, 0, 0)} for s, span in zip(SHIFTS, SPAN)
        ]
        needed[HOME] = {0, 1, 2}

        def shift(i):
            for k in range(3):
                for rows in halves:
                    ref = ext.at[k] if source is None else chain.at[source, k]
                    for t, value in enumerate(shifted([ref[t, rows, :] for t in tiles], i)):
                        sh[i, t, k, rows, :] = value
                    if masked and k in needed[i]:
                        for t, value in enumerate(shifted([words[k, t, rows, :] for t in tiles], i)):
                            sword[i, t, k, rows, :] = value

        def present(i, dx, t, rt):
            d = (dx, *SHIFTS[i])
            if d > (0, 0, 0):
                c, m = FLAGS[d]
                word = sword[HOME, t, c, pl.ds(2 + 4 * rt, 8), :]
            else:
                c, m = FLAGS[tuple(-v for v in d)]
                word = sword[i, t, c, pl.ds(2 + 4 * rt + dx, 8), :]
            return (word & (1 << m)) != 0

        sides = [(t, rt) for t in range(2) for rt in range(1 if last else 2)]
        acc = {side: [None] * 3 for side in sides}

        def compute(i):
            for j, dx in enumerate(SPAN[i]):
                n = FIRST[i] + j
                for t, rt in sides:
                    v = [sh[i, t, k, pl.ds(dx + 2 + 4 * rt, 8), :] for k in range(3)]
                    u = [coef[t, rt, n, k] for k in range(3)]
                    iso = coef[t, rt, n, 3]
                    if masked:
                        there = present(i, dx, t, rt)
                        u = [jnp.where(there, value, 0.0) for value in u]
                        iso = jnp.where(there, iso, 0.0)
                        for k, value in enumerate((*u, iso)):
                            coef[t, rt, n, k] = value
                    dot = u[0] * v[0] + u[1] * v[1] + u[2] * v[2]
                    for k in range(3):
                        term = u[k] * dot - iso * v[k]
                        old = acc[t, rt][k]
                        acc[t, rt][k] = term if old is None else old + term

        in_order(shift, compute)
        for t, rt in sides:
            scale = polo[t, pl.ds(2 + 4 * rt, 8), :]
            for k in range(3):
                out = acc[t, rt][k] * scale
                chain[target, k, t, pl.ds(2 + 4 * rt, 8), :] = out
                if not last:
                    if rt == 0:
                        chain[target, k, t, 14:16, :] = out[0:2]
                    else:
                        chain[target, k, t, 0:2, :] = out[6:8]

    def pack(index):
        parts = []
        for k in range(3):
            a = OWN - EDGE * k
            r = [roll(chain[index, k, t, 2:10, :], -a) for t in range(2)]
            parts.append(jnp.where(lane < LANES - a, r[0], r[1]))
        out = jnp.where(zone[0][0], parts[0], jnp.where(zone[0][1], parts[1], parts[2]))
        return jnp.where(packed, out, 0.0)

    pl.semaphore_wait(barrier, len(greeted))
    halo_start(0, send0.at[:, real], lambda b: recv0.at[b, :, real])
    halo_start(3, sendf.at[:, real], lambda b: recvf.at[b, :, real], lambda o: o[0] == 0 or o == (1, 0, 0))
    chain[...] = jnp.zeros_like(chain)
    halo_all(0).wait_recv()

    for k in range(3):
        assemble(lambda b: recv0[b, 0], k, geo.at[k])
        assemble(lambda b: recv0[b, 1], k, ext.at[k])
    assemble(lambda b: recv0[b, 2], 0, geo.at[4], 1.0)
    geo[3] = lax.rsqrt(geo[4])
    for half in range(2):
        rows = pl.ds(8 * half, 8)
        r = [roll(geo[4, t, rows, :], -ORIGIN) for t in range(3)]
        for t in range(2):
            polo[t, rows, :] = jnp.where(lane < LANES - ORIGIN, r[t], r[t + 1])

    def geometry(t, carry):
        def shift(i):
            a = ORIGIN + SHIFTS[i][0] * WIDE + SHIFTS[i][1]
            for rows in halves:
                for k in range(4):
                    pair = [roll(geo[k, t + u, rows, :], -a) for u in range(2)]
                    sgeo[i, t, k, rows, :] = jnp.where(lane < LANES - a, pair[0], pair[1])

        def compute(i):
            for rt in range(2):
                base = 2 + 4 * rt
                for j, dx in enumerate(SPAN[i]):
                    n = FIRST[i] + j
                    d = (dx, *SHIFTS[i])
                    rows = pl.ds(base + dx, 8)
                    sep = [sgeo[i, t, k, rows, :] - sgeo[HOME, t, k, pl.ds(base, 8), :] for k in range(3)]
                    sep = [v + e * site_spacing if e else v for v, e in zip(sep, d)]
                    sq = sep[0] * sep[0] + sep[1] * sep[1] + sep[2] * sep[2]
                    inv = lax.rsqrt(sq)
                    roots = sgeo[HOME, t, 3, pl.ds(base, 8), :] * sgeo[i, t, 3, rows, :]
                    damp = (thole_damping * roots) * (sq * (sq * inv))
                    fall = jnp.exp(-damp)
                    inv2 = inv * inv
                    inv3 = inv2 * inv
                    rad = (1.0 - (1.0 + damp) * fall) * (3.0 * inv3 * inv2)
                    root = rad * lax.rsqrt(rad)
                    for k in range(3):
                        coef[t, rt, n, k] = root * sep[k]
                    coef[t, rt, n, 3] = (1.0 - fall) * inv3

        in_order(shift, compute)
        return carry

    lax.fori_loop(0, 2, geometry, 0)

    halo_all(3).wait_recv()
    for b in range(9):
        if b != own:
            pltpu.make_async_remote_copy(
                src_ref=recvf.at[b, :, real], dst_ref=recvf.at[9 + b, :, real],
                send_sem=halo_send.at[4], recv_sem=halo_recv.at[4],
                device_id=at(1, 0, 0), device_id_type=MESH,
            ).start()
    flagged = []
    for b in range(18):
        if b == 9:
            halo_all(4).wait_recv()
        total = jnp.where(zone[0][0], 0.0, recv0[b, 2]) * float(2 ** FLAG_TILES)
        for n in range(FLAG_TILES):
            total = total + recvf[b, n] * float(2 ** n)
        flagged.append(total.astype(jnp.int32))
    for k in range(3):
        assemble(lambda b: flagged[b], k, words.at[k], 0)

    def dots_start(index, vectors, number):
        line = jnp.zeros((1, LANES), f32)
        for m in range(number):
            value = weight * vectors[m // 2] * vectors[(m + 1) // 2]
            value = jnp.sum(jnp.sum(value, axis=0, keepdims=True), axis=1, keepdims=True)
            line = jnp.where(pick == m, value, line)
        dot_src[index] = line
        dot_dst[index, rank] = line
        for o in others:
            pltpu.make_async_remote_copy(
                src_ref=dot_src.at[index], dst_ref=dot_dst.at[index, rank],
                send_sem=dot_send.at[index], recv_sem=dot_recv.at[index],
                device_id=at(*o), device_id_type=MESH,
            ).start()

    def dots_all(index):
        some = dot_dst.at[index, pl.ds(0, count - 1)]
        return pltpu.make_async_remote_copy(
            src_ref=some, dst_ref=some, send_sem=dot_send.at[index], recv_sem=dot_recv.at[index],
            device_id=at(1, 0, 0), device_id_type=MESH,
        )

    def dots_finish(index, number):
        dots_all(index).wait_recv()
        line = jnp.sum(dot_dst[index, :, 0, :], axis=0, keepdims=True)
        return [
            jnp.broadcast_to(jnp.sum(jnp.where(pick == m, line, 0.0), axis=1, keepdims=True), (ROWS, LANES))
            for m in range(number)
        ]

    def scalars(moments, history, steps):
        number = 2 * steps
        before = [0.0] * number
        if history:
            _, _, mu1, eta1, inv1, _ = history[-1]
            _, _, mu2, eta2, inv2, _ = history[-2]
            before[1] = moments[0] * inv1
            before[2] = moments[1] * inv1 + mu1 * before[1]
            older2 = before[1] * inv2
            before[3] = moments[2] * inv1 + mu1 * before[2] + eta1 * older2
            older3 = before[2] * inv2 + mu2 * older2
            before[4] = moments[3] * inv1 + mu1 * before[3] + eta1 * older3
        now, lead, seen = list(moments), None, 0.0
        out = []
        known = list(history)
        for i in range(steps):
            gamma = now[i] if lead is None else lead * now[i]
            if known:
                eta = gamma * known[-1][4] / known[-1][5]
                beta = eta * known[-1][0]
            else:
                eta = beta = jnp.zeros((ROWS, LANES), f32)
            ratio = now[i + 1] / now[i]
            mu = ratio - seen
            seen = ratio
            inv = 1.0 - mu - eta
            alpha = 1.0 / inv
            later = [0.0] * number
            for m in range(i + 1, number - 1 - i):
                later[m] = alpha * (now[m + 1] - mu * now[m] - eta * before[m])
            before, now = now, later
            lead = alpha if lead is None else lead * alpha
            out.append((alpha, beta, mu, eta, inv, gamma))
            known.append(out[-1])
        return out

    known = []
    table = [[]]

    def lanczos(vectors):
        i = len(table) - 1
        alpha, _, mu, eta, _, _ = known[i]
        now = table[i]
        table.append([
            alpha * (now[m + 1] - mu * now[m] - (eta * table[i - 1][m] if i else 0.0))
            for m in range(vectors)
        ])

    def chain_of_three(powers, first=False, between=None):
        for k in range(3):
            if k == 2 and between is not None:
                between()
            apply(None if k == 0 else k - 1, k, k == 2, first and k == 0)
            powers.append(pack(k))

    def share(index, value):
        send1[index] = value
        recv1[index, own] = value
        halo_start(1 + index, send1.at[index, real], lambda b: recv1.at[index, b, real])

    def receive(index):
        halo_all(1 + index).wait_recv()
        for k in range(3):
            assemble(lambda b: recv1[index, b], k, ext.at[k])

    def after_first():
        known.extend(scalars(dots_finish(0, 4), known, 2))

    def after_second():
        known.extend(scalars(dots_finish(1, 6), known, 3))

    chain_of_three(table[0], first=True)
    share(0, table[0][2])
    dots_start(0, table[0], 4)
    receive(0)
    chain_of_three(table[0], between=after_first)
    lanczos(5)
    lanczos(4)
    share(1, table[2][3])
    dots_start(1, table[2], 6)
    receive(1)
    chain_of_three(table[2], between=after_second)
    table[1].append(table[2][4] * known[1][4] + known[1][2] * table[1][4] + known[1][3] * table[0][4])
    for vectors in (6, 5, 4):
        lanczos(vectors)
    dots_start(2, table[5], 6)
    known += scalars(dots_finish(2, 6), known, 3)
    for vectors in (3, 2, 1):
        lanczos(vectors)

    line = jnp.zeros((1, LANES), f32)
    p = None
    for i, (alpha, beta, *_) in enumerate(known):
        p = table[i][0] if p is None else table[i][0] + beta * p
        x = x + alpha * p
        line = jnp.where(pick == i, alpha[0:1], line)
    residual = table[ITERS][0] * weight
    out_ref[0] = x
    out_ref[1] = residual
    out_ref[2, 0:1, :] = line

    for index in range(5):
        halo_all(index).wait_send()
    for index in range(3):
        dots_all(index).wait_send()


def unpack(in_ref, x_out, r_out, len_out):
    for k, ref in enumerate((x_out, r_out)):
        value = in_ref[k]
        for y in range(EDGE):
            for c in range(3):
                ref[:, y, c, :] = roll(value, -(y * WIDE + c * EDGE))[:EDGE, :EDGE]
    len_out[...] = in_ref[2, 0:1, :ITERS]


def solution(mesh):
    sizes = tuple(mesh.shape[a] for a in ("gx", "gy", "gz"))
    assert sizes[0] == 2
    count = sizes[0] * sizes[1] * sizes[2]

    def local(permanent_field, polar, jitter, neighbors):
        assert polar.shape == (EDGE, EDGE, EDGE)
        vmem = pl.BlockSpec(memory_space=pltpu.VMEM)
        shape = jax.ShapeDtypeStruct((EDGE, EDGE, 3, EDGE), f32)
        wide, near = (3, 16, LANES), (2, 16, LANES)
        shifts = len(SHIFTS)
        anywhere = pl.BlockSpec(memory_space=pl.ANY)
        packed = pl.pallas_call(
            functools.partial(kernel, sizes),
            out_shape=pltpu.VMEM((3, ROWS, LANES), f32),
            in_specs=[anywhere] * 4,
            out_specs=vmem,
            scratch_shapes=[
                pltpu.VMEM((EDGE, EDGE, 3, EDGE), f32),
                pltpu.VMEM((EDGE, EDGE, EDGE), f32),
                pltpu.VMEM((EDGE, EDGE, 3, EDGE), f32),
                pltpu.VMEM(neighbors.shape, jnp.int32),
                pltpu.VMEM((3, *wide), f32),
                pltpu.VMEM((shifts, 2, 3, 16, LANES), f32),
                pltpu.VMEM((5, *wide), f32),
                pltpu.VMEM((3, *wide), jnp.int32),
                pltpu.VMEM((shifts, 2, 4, 16, LANES), f32),
                pltpu.VMEM((shifts, 2, 3, 16, LANES), jnp.int32),
                pltpu.VMEM(near, f32),
                pltpu.VMEM((2, 2, len(STENCIL), 4, ROWS, LANES), f32),
                pltpu.VMEM((3, 3, *near), f32),
                pltpu.VMEM((TILES, ROWS, LANES), f32),
                pltpu.VMEM((18, TILES, ROWS, LANES), f32),
                pltpu.VMEM((FLAG_TILES, ROWS, LANES), f32),
                pltpu.VMEM((18, FLAG_TILES, ROWS, LANES), f32),
                pltpu.VMEM((2, ROWS, LANES), f32),
                pltpu.VMEM((2, 18, ROWS, LANES), f32),
                pltpu.VMEM((3, 1, LANES), f32),
                pltpu.VMEM((3, count, 1, LANES), f32),
                pltpu.SemaphoreType.DMA((5,)),
                pltpu.SemaphoreType.DMA((5,)),
                pltpu.SemaphoreType.DMA((3,)),
                pltpu.SemaphoreType.DMA((3,)),
                pltpu.SemaphoreType.DMA((4,)),
            ],
            compiler_params=pltpu.CompilerParams(collective_id=0, has_side_effects=True),
        )(
            jnp.moveaxis(permanent_field, -1, 2),
            polar,
            jnp.moveaxis(jitter, -1, 2),
            neighbors,
        )
        x, r, steps = pl.pallas_call(
            unpack,
            out_shape=(shape, shape, jax.ShapeDtypeStruct((1, ITERS), f32)),
            in_specs=[vmem],
            out_specs=(vmem, vmem, vmem),
        )(pltpu.with_memory_space_constraint(packed, pltpu.VMEM))
        return jnp.moveaxis(x, 2, -1), jnp.moveaxis(r, 2, -1), steps.reshape(ITERS)

    return jax.shard_map(
        local,
        mesh=mesh,
        in_specs=(
            P("gx", "gy", "gz", None),
            P("gx", "gy", "gz"),
            P("gx", "gy", "gz", None),
            P("gx", "gy", "gz", None),
        ),
        out_specs=(P("gx", "gy", "gz", None), P("gx", "gy", "gz", None), P()),
        check_vma=False,
    )
```

```python
import functools

import jax
import jax.numpy as jnp
from jax import lax
from jax.experimental import pallas as pl
from jax.experimental.pallas import tpu as pltpu
from jax.sharding import PartitionSpec as P

ITERS = 8
MESH = pl.DeviceIdType.MESH
thole_damping = 0.39
site_spacing = 3.5
ROWS, LANES = 8, 128
EDGE = 6
WIDE = 3 * EDGE
ORIGIN = 2 * WIDE + 2
OWN = EDGE * WIDE + EDGE - ORIGIN
f32 = jnp.float32

STENCIL = [
    (a, b, c)
    for a in range(-2, 3)
    for b in range(-2, 3)
    for c in range(-2, 3)
    if 1 <= a * a + b * b + c * c <= 5
]
SHIFTS = sorted({(b, c) for a, b, c in STENCIL})
SPAN = [[d[0] for d in STENCIL if d[1:] == s] for s in SHIFTS]
FIRST = [sum(len(v) for v in SPAN[:i]) for i in range(len(SHIFTS))]
HOME = SHIFTS.index((0, 0))
FORWARD = [d for d in STENCIL if d > (0, 0, 0)]


def flag_places():
    room = {0: 9, 1: 10, 2: 10}
    used = {0: 0, 1: 0, 2: 0}
    places = {}
    for d in FORWARD:
        c = d[0] if used[d[0]] < room[d[0]] else 2
        if d[0] != 2 and used[d[0]] >= room[d[0]]:
            c = 2
        places[d] = (c, used[c])
        used[c] += 1
    assert used[2] <= room[2]
    return places


FLAGS = flag_places()
FLAG_TILES = 9
TILES = 3
GREET_Y = (0, 1, 3)
GREET_Z = (0, 1, 4, 7, 9, 12, 15)


def roll(value, shift):
    shift = shift % LANES
    return value if shift == 0 else pltpu.roll(value, shift, axis=1)


def kernel(
    sizes,
    field_in, pol_in, jit_in, nb_in, out_ref,
    field_ref, pol_ref, jit_ref, nb_ref,
    ext, sh, geo, words, sgeo, sword, polo, coef, chain,
    send0, recv0, sendf, recvf, send1, recv1, dot_src, dot_dst,
    halo_send, halo_recv, dot_send, dot_recv, in_sems,
):
    nx, ny, nz = sizes
    count = nx * ny * nz
    gx, gy, gz = lax.axis_index("gx"), lax.axis_index("gy"), lax.axis_index("gz")
    rank = (gx * ny + gy) * nz + gz

    def at(ox, oy, oz):
        return (lax.rem(gx + ox + nx, nx), lax.rem(gy + oy + ny, ny), lax.rem(gz + oz + nz, nz))

    others = [
        (a, b, c) for a in range(nx) for b in range(ny) for c in range(nz) if (a, b, c) != (0, 0, 0)
    ]

    def hops(o):
        ring = lambda v: min(v % 4, -v % 4)
        along = max(ring(o[2] // 4), ring(o[2] // 4 + 1)) if o[2] % 4 else ring(o[2] // 4)
        return 4 * (ring(o[1]) + ring(o[2] % 4) + along) + o[0]

    others.sort(key=lambda o: -hops(o))

    barrier = pltpu.get_barrier_semaphore()
    loads = [
        pltpu.make_async_copy(source, target, in_sems.at[k])
        for k, (source, target) in enumerate((
            (nb_in, nb_ref), (field_in, field_ref), (pol_in, pol_ref), (jit_in, jit_ref),
        ))
    ]
    for load in loads:
        load.start()
    greeted = [o for o in others if o[1] in GREET_Y and o[2] in GREET_Z]
    for o in greeted:
        pl.semaphore_signal(barrier, inc=1, device_id=at(*o), device_id_type=MESH)
    lane = lax.broadcasted_iota(jnp.int32, (ROWS, LANES), 1)
    row = lax.broadcasted_iota(jnp.int32, (ROWS, LANES), 0)
    pick = lax.broadcasted_iota(jnp.int32, (1, LANES), 1)

    def third(b):
        position = lax.rem(lane - 108 * b + 2 * LANES * 2, LANES)
        within = position - (position // WIDE) * WIDE
        return within < EDGE, within < 2 * EDGE

    zone = [third(b) for b in range(3)]
    packed = (row < EDGE) & (lane < EDGE * WIDE)

    def gather3(ref, comps):
        out = jnp.zeros((ROWS, LANES), f32)
        for y in range(EDGE):
            for c in range(comps):
                part = ref[:, y, c, :] if comps == 3 else ref[:, y, :]
                part = jnp.concatenate([part, jnp.zeros((EDGE, LANES - EDGE), f32)], axis=1)
                part = jnp.concatenate([part, jnp.zeros((ROWS - EDGE, LANES), f32)], axis=0)
                out = out + roll(part, y * WIDE + c * EDGE)
        return out

    for load in loads:
        load.wait()
    field, jit = gather3(field_ref, 3), gather3(jit_ref, 3) * site_spacing
    pol0 = gather3(pol_ref, 1)
    polp = pol0 + roll(pol0, EDGE) + roll(pol0, 2 * EDGE)
    weight = jnp.where(packed, 1.0 / jnp.where(packed, polp, 1.0), 0.0)
    x = polp * field

    slots = nb_ref.shape[3]
    plane = lax.broadcasted_iota(jnp.int32, (EDGE, slots), 0) * 100
    spread = [jnp.zeros((ROWS, LANES), f32) for _ in range(3)]
    for y in range(EDGE):
        for z in range(EDGE):
            entry = nb_ref[:, y, z, :]
            code = entry - plane - (222 + 10 * y + z)
            real = code > 0
            code = code + 22
            dx = jnp.where(code >= 200, 2, jnp.where(code >= 100, 1, 0))
            rem = code - dx * 100
            bit = rem - 5 * ((rem * 205) >> 11) - 2
            value = jnp.where(real, jnp.left_shift(1, jnp.where(real, bit, 0)), 0).astype(f32)
            for k in range(3):
                total = jnp.sum(jnp.where(dx == k, value, 0.0), axis=1, keepdims=True)
                total = jnp.concatenate([total, jnp.zeros((ROWS - EDGE, 1), f32)], axis=0)
                spread[k] = spread[k] + jnp.where(lane == y * WIDE + k * EDGE + z, total, 0.0)
    bits = [s.astype(jnp.int32) for s in spread]
    moved = {}

    def flag_tile(n):
        out = jnp.zeros((ROWS, LANES), jnp.int32)
        for d, (c, m) in FLAGS.items():
            if m == n:
                key = (d[0], c)
                if key not in moved:
                    moved[key] = roll(bits[d[0]], (c - d[0]) * EDGE)
                out = out | (lax.shift_right_logical(moved[key], 5 * (d[1] + 2) + d[2]) & 1)
        return out.astype(f32)

    send0[0] = jit
    send0[1] = pol0 + flag_tile(FLAG_TILES)
    send0[2] = x
    for n in range(FLAG_TILES):
        sendf[n] = flag_tile(n)
    own = 4
    recv0[own] = send0[...]
    recvf[own] = sendf[...]

    real = pl.ds(0, EDGE)

    def halo_start(index, src, get_dst, wanted=lambda o: True):
        for oy in (-1, 1, 0):
            for oz in (-1, 1, 0):
                for ox in (1, 0):
                    if (ox, oy, oz) == (0, 0, 0) or not wanted((ox, oy, oz)):
                        continue
                    back = ox * 9 + (1 - oy) * 3 + 1 - oz
                    pltpu.make_async_remote_copy(
                        src_ref=src, dst_ref=get_dst(back),
                        send_sem=halo_send.at[index], recv_sem=halo_recv.at[index],
                        device_id=at(ox, oy, oz), device_id_type=MESH,
                    ).start()

    def halo_all(index):
        some = pl.ds(0, 17)
        ref = {
            0: recv0.at[some, pl.ds(0, 2), real], 5: recv0.at[some, pl.ds(2, 1), real],
            3: recvf.at[pl.ds(0, 9), :, real], 4: recvf.at[pl.ds(0, 8), :, real],
            1: recv1.at[0, some, real], 2: recv1.at[1, some, real],
        }[index]
        return pltpu.make_async_remote_copy(
            src_ref=ref, dst_ref=ref, send_sem=halo_send.at[index], recv_sem=halo_recv.at[index],
            device_id=at(1, 0, 0), device_id_type=MESH,
        )

    def assemble(get, c, target, fill=0.0):
        full = []
        for h in range(2):
            part = []
            for b in range(3):
                m = [roll(get(h * 9 + b * 3 + k), 108 * b + EDGE * (k - c)) for k in range(3)]
                part.append(jnp.where(zone[b][0], m[0], jnp.where(zone[b][1], m[1], m[2])))
            full.append((
                jnp.where(lane < 108, part[0], part[1]),
                jnp.where(lane < 88, part[1], part[2]),
                jnp.where(lane < 68, part[2], fill),
            ))
        for t in range(3):
            target[t, 2:8, :] = full[0][t][:6]
            target[t, 8:14, :] = full[1][t][:6]
            target[t, 0:2, :] = full[1][t][4:6]
            target[t, 14:16, :] = full[0][t][:2]

    def shifted(v, i):
        dy, dz = SHIFTS[i]
        s = dy * WIDE + dz + (ORIGIN if len(v) == 3 else 0)
        if s == 0:
            return v
        r = [roll(u, -s) for u in v]
        if len(v) == 3:
            return [jnp.where(lane < LANES - s, r[t], r[t + 1]) for t in range(2)]
        if s > 0:
            return [jnp.where(lane < LANES - s, r[0], r[1]), r[1]]
        return [r[0], jnp.where(lane >= -s, r[1], r[0])]

    halves = (pl.ds(0, 8), pl.ds(8, 8))

    def in_order(shift, compute, ahead=4):
        order = [HOME] + [i for i in range(len(SHIFTS)) if i != HOME]
        for place in range(len(order) + ahead):
            if place < len(order):
                shift(order[place])
            if place >= ahead:
                compute(order[place - ahead])

    def apply(source, target, last, masked=False):
        tiles = range(3) if source is None else range(2)
        needed = [
            {FLAGS[tuple(-v for v in (dx, *s))][0] for dx in span if (dx, *s) < (0, 0, 0)} for s, span in zip(SHIFTS, SPAN)
        ]
        needed[HOME] = {0, 1, 2}

        def shift(i):
            for k in range(3):
                for rows in halves:
                    ref = ext.at[k] if source is None else chain.at[source, k]
                    for t, value in enumerate(shifted([ref[t, rows, :] for t in tiles], i)):
                        sh[i, t, k, rows, :] = value
                    if masked and k in needed[i]:
                        for t, value in enumerate(shifted([words[k, t, rows, :] for t in tiles], i)):
                            sword[i, t, k, rows, :] = value

        def present(i, dx, t, rt):
            d = (dx, *SHIFTS[i])
            if d > (0, 0, 0):
                c, m = FLAGS[d]
                word = sword[HOME, t, c, pl.ds(2 + 4 * rt, 8), :]
            else:
                c, m = FLAGS[tuple(-v for v in d)]
                word = sword[i, t, c, pl.ds(2 + 4 * rt + dx, 8), :]
            return (word & (1 << m)) != 0

        sides = [(t, rt) for t in range(2) for rt in range(1 if last else 2)]
        acc = {side: [None] * 3 for side in sides}

        def compute(i):
            for j, dx in enumerate(SPAN[i]):
                n = FIRST[i] + j
                for t, rt in sides:
                    v = [sh[i, t, k, pl.ds(dx + 2 + 4 * rt, 8), :] for k in range(3)]
                    u = [coef[t, rt, n, k] for k in range(3)]
                    iso = coef[t, rt, n, 3]
                    if masked:
                        there = present(i, dx, t, rt)
                        u = [jnp.where(there, value, 0.0) for value in u]
                        iso = jnp.where(there, iso, 0.0)
                        for k, value in enumerate((*u, iso)):
                            coef[t, rt, n, k] = value
                    dot = u[0] * v[0] + u[1] * v[1] + u[2] * v[2]
                    for k in range(3):
                        term = u[k] * dot - iso * v[k]
                        old = acc[t, rt][k]
                        acc[t, rt][k] = term if old is None else old + term

        in_order(shift, compute)
        for t, rt in sides:
            scale = polo[t, pl.ds(2 + 4 * rt, 8), :]
            for k in range(3):
                out = acc[t, rt][k] * scale
                chain[target, k, t, pl.ds(2 + 4 * rt, 8), :] = out
                if not last:
                    if rt == 0:
                        chain[target, k, t, 14:16, :] = out[0:2]
                    else:
                        chain[target, k, t, 0:2, :] = out[6:8]

    def pack(index):
        parts = []
        for k in range(3):
            a = OWN - EDGE * k
            r = [roll(chain[index, k, t, 2:10, :], -a) for t in range(2)]
            parts.append(jnp.where(lane < LANES - a, r[0], r[1]))
        out = jnp.where(zone[0][0], parts[0], jnp.where(zone[0][1], parts[1], parts[2]))
        return jnp.where(packed, out, 0.0)

    pl.semaphore_wait(barrier, len(greeted))
    early, late = pl.ds(0, 2), pl.ds(2, 1)
    halo_start(0, send0.at[early, real], lambda b: recv0.at[b, early, real])
    halo_start(3, sendf.at[:, real], lambda b: recvf.at[b, :, real], lambda o: o[0] == 0 or o == (1, 0, 0))
    halo_start(5, send0.at[late, real], lambda b: recv0.at[b, late, real])
    chain[...] = jnp.zeros_like(chain)
    halo_all(0).wait_recv()

    for k in range(3):
        assemble(lambda b: recv0[b, 0], k, geo.at[k])
    assemble(lambda b: recv0[b, 1], 0, geo.at[4], 1.0)
    geo[3] = lax.rsqrt(geo[4])
    for half in range(2):
        rows = pl.ds(8 * half, 8)
        r = [roll(geo[4, t, rows, :], -ORIGIN) for t in range(3)]
        for t in range(2):
            polo[t, rows, :] = jnp.where(lane < LANES - ORIGIN, r[t], r[t + 1])

    def geometry(t, carry):
        def shift(i):
            a = ORIGIN + SHIFTS[i][0] * WIDE + SHIFTS[i][1]
            for rows in halves:
                for k in range(4):
                    pair = [roll(geo[k, t + u, rows, :], -a) for u in range(2)]
                    sgeo[i, t, k, rows, :] = jnp.where(lane < LANES - a, pair[0], pair[1])

        def compute(i):
            for rt in range(2):
                base = 2 + 4 * rt
                for j, dx in enumerate(SPAN[i]):
                    n = FIRST[i] + j
                    d = (dx, *SHIFTS[i])
                    rows = pl.ds(base + dx, 8)
                    sep = [sgeo[i, t, k, rows, :] - sgeo[HOME, t, k, pl.ds(base, 8), :] for k in range(3)]
                    sep = [v + e * site_spacing if e else v for v, e in zip(sep, d)]
                    sq = sep[0] * sep[0] + sep[1] * sep[1] + sep[2] * sep[2]
                    inv = lax.rsqrt(sq)
                    roots = sgeo[HOME, t, 3, pl.ds(base, 8), :] * sgeo[i, t, 3, rows, :]
                    damp = (thole_damping * roots) * (sq * (sq * inv))
                    fall = jnp.exp(-damp)
                    inv2 = inv * inv
                    inv3 = inv2 * inv
                    rad = (1.0 - (1.0 + damp) * fall) * (3.0 * inv3 * inv2)
                    root = rad * lax.rsqrt(rad)
                    for k in range(3):
                        coef[t, rt, n, k] = root * sep[k]
                    coef[t, rt, n, 3] = (1.0 - fall) * inv3

        in_order(shift, compute)
        return carry

    lax.fori_loop(0, 2, geometry, 0)

    halo_all(3).wait_recv()
    for b in range(9):
        if b != own:
            pltpu.make_async_remote_copy(
                src_ref=recvf.at[b, :, real], dst_ref=recvf.at[9 + b, :, real],
                send_sem=halo_send.at[4], recv_sem=halo_recv.at[4],
                device_id=at(1, 0, 0), device_id_type=MESH,
            ).start()
    flagged = []
    for b in range(18):
        if b == 9:
            halo_all(4).wait_recv()
        total = jnp.where(zone[0][0], 0.0, recv0[b, 1]) * float(2 ** FLAG_TILES)
        for n in range(FLAG_TILES):
            total = total + recvf[b, n] * float(2 ** n)
        flagged.append(total.astype(jnp.int32))
    for k in range(3):
        assemble(lambda b: flagged[b], k, words.at[k], 0)
    halo_all(5).wait_recv()
    for k in range(3):
        assemble(lambda b: recv0[b, 2], k, ext.at[k])

    def dots_start(index, vectors, number):
        line = jnp.zeros((1, LANES), f32)
        for m in range(number):
            value = weight * vectors[m // 2] * vectors[(m + 1) // 2]
            value = jnp.sum(jnp.sum(value, axis=0, keepdims=True), axis=1, keepdims=True)
            line = jnp.where(pick == m, value, line)
        dot_src[index] = line
        dot_dst[index, rank] = line
        for o in others:
            pltpu.make_async_remote_copy(
                src_ref=dot_src.at[index], dst_ref=dot_dst.at[index, rank],
                send_sem=dot_send.at[index], recv_sem=dot_recv.at[index],
                device_id=at(*o), device_id_type=MESH,
            ).start()

    def dots_all(index):
        some = dot_dst.at[index, pl.ds(0, count - 1)]
        return pltpu.make_async_remote_copy(
            src_ref=some, dst_ref=some, send_sem=dot_send.at[index], recv_sem=dot_recv.at[index],
            device_id=at(1, 0, 0), device_id_type=MESH,
        )

    def dots_finish(index, number):
        dots_all(index).wait_recv()
        line = jnp.sum(dot_dst[index, :, 0, :], axis=0, keepdims=True)
        return [
            jnp.broadcast_to(jnp.sum(jnp.where(pick == m, line, 0.0), axis=1, keepdims=True), (ROWS, LANES))
            for m in range(number)
        ]

    def scalars(moments, history, steps):
        number = 2 * steps
        before = [0.0] * number
        if history:
            _, _, mu1, eta1, inv1, _ = history[-1]
            _, _, mu2, eta2, inv2, _ = history[-2]
            before[1] = moments[0] * inv1
            before[2] = moments[1] * inv1 + mu1 * before[1]
            older2 = before[1] * inv2
            before[3] = moments[2] * inv1 + mu1 * before[2] + eta1 * older2
            older3 = before[2] * inv2 + mu2 * older2
            before[4] = moments[3] * inv1 + mu1 * before[3] + eta1 * older3
        now, lead, seen = list(moments), None, 0.0
        out = []
        known = list(history)
        for i in range(steps):
            gamma = now[i] if lead is None else lead * now[i]
            if known:
                eta = gamma * known[-1][4] / known[-1][5]
                beta = eta * known[-1][0]
            else:
                eta = beta = jnp.zeros((ROWS, LANES), f32)
            ratio = now[i + 1] / now[i]
            mu = ratio - seen
            seen = ratio
            inv = 1.0 - mu - eta
            alpha = 1.0 / inv
            later = [0.0] * number
            for m in range(i + 1, number - 1 - i):
                later[m] = alpha * (now[m + 1] - mu * now[m] - eta * before[m])
            before, now = now, later
            lead = alpha if lead is None else lead * alpha
            out.append((alpha, beta, mu, eta, inv, gamma))
            known.append(out[-1])
        return out

    known = []
    table = [[]]

    def lanczos(vectors):
        i = len(table) - 1
        alpha, _, mu, eta, _, _ = known[i]
        now = table[i]
        table.append([
            alpha * (now[m + 1] - mu * now[m] - (eta * table[i - 1][m] if i else 0.0))
            for m in range(vectors)
        ])

    def chain_of_three(powers, first=False, between=None):
        for k in range(3):
            if k == 2 and between is not None:
                between()
            apply(None if k == 0 else k - 1, k, k == 2, first and k == 0)
            powers.append(pack(k))

    def share(index, value):
        send1[index] = value
        recv1[index, own] = value
        halo_start(1 + index, send1.at[index, real], lambda b: recv1.at[index, b, real])

    def receive(index):
        halo_all(1 + index).wait_recv()
        for k in range(3):
            assemble(lambda b: recv1[index, b], k, ext.at[k])

    def after_first():
        known.extend(scalars(dots_finish(0, 4), known, 2))

    def after_second():
        known.extend(scalars(dots_finish(1, 6), known, 3))

    chain_of_three(table[0], first=True)
    share(0, table[0][2])
    dots_start(0, table[0], 4)
    receive(0)
    chain_of_three(table[0], between=after_first)
    lanczos(5)
    lanczos(4)
    share(1, table[2][3])
    dots_start(1, table[2], 6)
    receive(1)
    chain_of_three(table[2], between=after_second)
    table[1].append(table[2][4] * known[1][4] + known[1][2] * table[1][4] + known[1][3] * table[0][4])
    for vectors in (6, 5, 4):
        lanczos(vectors)
    dots_start(2, table[5], 6)
    known += scalars(dots_finish(2, 6), known, 3)
    for vectors in (3, 2, 1):
        lanczos(vectors)

    line = jnp.zeros((1, LANES), f32)
    p = None
    for i, (alpha, beta, *_) in enumerate(known):
        p = table[i][0] if p is None else table[i][0] + beta * p
        x = x + alpha * p
        line = jnp.where(pick == i, alpha[0:1], line)
    residual = table[ITERS][0] * weight
    out_ref[0] = x
    out_ref[1] = residual
    out_ref[2, 0:1, :] = line

    for index in range(6):
        halo_all(index).wait_send()
    for index in range(3):
        dots_all(index).wait_send()


def unpack(in_ref, x_out, r_out, len_out):
    for k, ref in enumerate((x_out, r_out)):
        value = in_ref[k]
        for y in range(EDGE):
            for c in range(3):
                ref[:, y, c, :] = roll(value, -(y * WIDE + c * EDGE))[:EDGE, :EDGE]
    len_out[...] = in_ref[2, 0:1, :ITERS]


def solution(mesh):
    sizes = tuple(mesh.shape[a] for a in ("gx", "gy", "gz"))
    assert sizes[0] == 2
    count = sizes[0] * sizes[1] * sizes[2]

    def local(permanent_field, polar, jitter, neighbors):
        assert polar.shape == (EDGE, EDGE, EDGE)
        vmem = pl.BlockSpec(memory_space=pltpu.VMEM)
        shape = jax.ShapeDtypeStruct((EDGE, EDGE, 3, EDGE), f32)
        wide, near = (3, 16, LANES), (2, 16, LANES)
        shifts = len(SHIFTS)
        anywhere = pl.BlockSpec(memory_space=pl.ANY)
        packed = pl.pallas_call(
            functools.partial(kernel, sizes),
            out_shape=pltpu.VMEM((3, ROWS, LANES), f32),
            in_specs=[anywhere] * 4,
            out_specs=vmem,
            scratch_shapes=[
                pltpu.VMEM((EDGE, EDGE, 3, EDGE), f32),
                pltpu.VMEM((EDGE, EDGE, EDGE), f32),
                pltpu.VMEM((EDGE, EDGE, 3, EDGE), f32),
                pltpu.VMEM(neighbors.shape, jnp.int32),
                pltpu.VMEM((3, *wide), f32),
                pltpu.VMEM((shifts, 2, 3, 16, LANES), f32),
                pltpu.VMEM((5, *wide), f32),
                pltpu.VMEM((3, *wide), jnp.int32),
                pltpu.VMEM((shifts, 2, 4, 16, LANES), f32),
                pltpu.VMEM((shifts, 2, 3, 16, LANES), jnp.int32),
                pltpu.VMEM(near, f32),
                pltpu.VMEM((2, 2, len(STENCIL), 4, ROWS, LANES), f32),
                pltpu.VMEM((3, 3, *near), f32),
                pltpu.VMEM((TILES, ROWS, LANES), f32),
                pltpu.VMEM((18, TILES, ROWS, LANES), f32),
                pltpu.VMEM((FLAG_TILES, ROWS, LANES), f32),
                pltpu.VMEM((18, FLAG_TILES, ROWS, LANES), f32),
                pltpu.VMEM((2, ROWS, LANES), f32),
                pltpu.VMEM((2, 18, ROWS, LANES), f32),
                pltpu.VMEM((3, 1, LANES), f32),
                pltpu.VMEM((3, count, 1, LANES), f32),
                pltpu.SemaphoreType.DMA((6,)),
                pltpu.SemaphoreType.DMA((6,)),
                pltpu.SemaphoreType.DMA((3,)),
                pltpu.SemaphoreType.DMA((3,)),
                pltpu.SemaphoreType.DMA((4,)),
            ],
            compiler_params=pltpu.CompilerParams(collective_id=0, has_side_effects=True),
        )(
            jnp.moveaxis(permanent_field, -1, 2),
            polar,
            jnp.moveaxis(jitter, -1, 2),
            neighbors,
        )
        x, r, steps = pl.pallas_call(
            unpack,
            out_shape=(shape, shape, jax.ShapeDtypeStruct((1, ITERS), f32)),
            in_specs=[vmem],
            out_specs=(vmem, vmem, vmem),
        )(pltpu.with_memory_space_constraint(packed, pltpu.VMEM))
        return jnp.moveaxis(x, 2, -1), jnp.moveaxis(r, 2, -1), steps.reshape(ITERS)

    return jax.shard_map(
        local,
        mesh=mesh,
        in_specs=(
            P("gx", "gy", "gz", None),
            P("gx", "gy", "gz"),
            P("gx", "gy", "gz", None),
            P("gx", "gy", "gz", None),
        ),
        out_specs=(P("gx", "gy", "gz", None), P("gx", "gy", "gz", None), P()),
        check_vma=False,
    )
```

```python
import functools

import jax
import jax.numpy as jnp
from jax import lax
from jax.experimental import pallas as pl
from jax.experimental.pallas import tpu as pltpu
from jax.sharding import PartitionSpec as P

ITERS = 8
MESH = pl.DeviceIdType.MESH
thole_damping = 0.39
site_spacing = 3.5
ROWS, LANES = 8, 128
EDGE = 6
WIDE = 3 * EDGE
ORIGIN = 2 * WIDE + 2
OWN = EDGE * WIDE + EDGE - ORIGIN
f32 = jnp.float32

STENCIL = [
    (a, b, c)
    for a in range(-2, 3)
    for b in range(-2, 3)
    for c in range(-2, 3)
    if 1 <= a * a + b * b + c * c <= 5
]
SHIFTS = sorted({(b, c) for a, b, c in STENCIL})
SPAN = [[d[0] for d in STENCIL if d[1:] == s] for s in SHIFTS]
FIRST = [sum(len(v) for v in SPAN[:i]) for i in range(len(SHIFTS))]
HOME = SHIFTS.index((0, 0))
FORWARD = [d for d in STENCIL if d > (0, 0, 0)]


def flag_places():
    room = {0: 9, 1: 10, 2: 10}
    used = {0: 0, 1: 0, 2: 0}
    places = {}
    for d in FORWARD:
        c = d[0] if used[d[0]] < room[d[0]] else 2
        if d[0] != 2 and used[d[0]] >= room[d[0]]:
            c = 2
        places[d] = (c, used[c])
        used[c] += 1
    assert used[2] <= room[2]
    return places


FLAGS = flag_places()
FLAG_TILES = 9
TILES = 3
GREET_Y = (0, 1, 3)
GREET_Z = (0, 1, 4, 7, 9, 12, 15)


def roll(value, shift):
    shift = shift % LANES
    return value if shift == 0 else pltpu.roll(value, shift, axis=1)


def kernel(
    sizes,
    field_in, pol_in, jit_in, nb_in, out_ref,
    field_ref, pol_ref, jit_ref, nb_ref,
    ext, sh, geo, words, sgeo, sword, polo, coef, chain,
    send0, recv0, sendf, recvf, send1, recv1, dot_src, dot_dst,
    halo_send, halo_recv, dot_send, dot_recv, in_sems,
):
    nx, ny, nz = sizes
    count = nx * ny * nz
    gx, gy, gz = lax.axis_index("gx"), lax.axis_index("gy"), lax.axis_index("gz")
    rank = (gx * ny + gy) * nz + gz

    def at(ox, oy, oz):
        return (lax.rem(gx + ox + nx, nx), lax.rem(gy + oy + ny, ny), lax.rem(gz + oz + nz, nz))

    others = [
        (a, b, c) for a in range(nx) for b in range(ny) for c in range(nz) if (a, b, c) != (0, 0, 0)
    ]

    def hops(o):
        ring = lambda v: min(v % 4, -v % 4)
        along = max(ring(o[2] // 4), ring(o[2] // 4 + 1)) if o[2] % 4 else ring(o[2] // 4)
        return 4 * (ring(o[1]) + ring(o[2] % 4) + along) + o[0]

    others.sort(key=lambda o: -hops(o))

    barrier = pltpu.get_barrier_semaphore()
    loads = [
        pltpu.make_async_copy(source, target, in_sems.at[k])
        for k, (source, target) in enumerate((
            (nb_in, nb_ref), (field_in, field_ref), (pol_in, pol_ref), (jit_in, jit_ref),
        ))
    ]
    for load in loads:
        load.start()
    greeted = [o for o in others if o[2] in GREET_Z and (o[1] in GREET_Y[1:] or o[1] == 0 and o[2] in GREET_Z[::6] + (1,))]
    for o in greeted:
        pl.semaphore_signal(barrier, inc=1, device_id=at(*o), device_id_type=MESH)
    lane = lax.broadcasted_iota(jnp.int32, (ROWS, LANES), 1)
    row = lax.broadcasted_iota(jnp.int32, (ROWS, LANES), 0)
    pick = lax.broadcasted_iota(jnp.int32, (1, LANES), 1)

    def third(b):
        position = lax.rem(lane - 108 * b + 2 * LANES * 2, LANES)
        within = position - (position // WIDE) * WIDE
        return within < EDGE, within < 2 * EDGE

    zone = [third(b) for b in range(3)]
    packed = (row < EDGE) & (lane < EDGE * WIDE)

    def gather3(ref, comps):
        out = jnp.zeros((ROWS, LANES), f32)
        for y in range(EDGE):
            for c in range(comps):
                part = ref[:, y, c, :] if comps == 3 else ref[:, y, :]
                part = jnp.concatenate([part, jnp.zeros((EDGE, LANES - EDGE), f32)], axis=1)
                part = jnp.concatenate([part, jnp.zeros((ROWS - EDGE, LANES), f32)], axis=0)
                out = out + roll(part, y * WIDE + c * EDGE)
        return out

    for load in loads:
        load.wait()
    field, jit = gather3(field_ref, 3), gather3(jit_ref, 3) * site_spacing
    pol0 = gather3(pol_ref, 1)
    polp = pol0 + roll(pol0, EDGE) + roll(pol0, 2 * EDGE)
    weight = jnp.where(packed, 1.0 / jnp.where(packed, polp, 1.0), 0.0)
    x = polp * field

    slots = nb_ref.shape[3]
    plane = lax.broadcasted_iota(jnp.int32, (EDGE, slots), 0) * 100
    spread = [jnp.zeros((ROWS, LANES), f32) for _ in range(3)]
    for y in range(EDGE):
        for z in range(EDGE):
            entry = nb_ref[:, y, z, :]
            code = entry - plane - (222 + 10 * y + z)
            real = code > 0
            code = code + 22
            dx = jnp.where(code >= 200, 2, jnp.where(code >= 100, 1, 0))
            rem = code - dx * 100
            bit = rem - 5 * ((rem * 205) >> 11) - 2
            value = jnp.where(real, jnp.left_shift(1, jnp.where(real, bit, 0)), 0).astype(f32)
            for k in range(3):
                total = jnp.sum(jnp.where(dx == k, value, 0.0), axis=1, keepdims=True)
                total = jnp.concatenate([total, jnp.zeros((ROWS - EDGE, 1), f32)], axis=0)
                spread[k] = spread[k] + jnp.where(lane == y * WIDE + k * EDGE + z, total, 0.0)
    bits = [s.astype(jnp.int32) for s in spread]
    moved = {}

    def flag_tile(n):
        out = jnp.zeros((ROWS, LANES), jnp.int32)
        for d, (c, m) in FLAGS.items():
            if m == n:
                key = (d[0], c)
                if key not in moved:
                    moved[key] = roll(bits[d[0]], (c - d[0]) * EDGE)
                out = out | (lax.shift_right_logical(moved[key], 5 * (d[1] + 2) + d[2]) & 1)
        return out.astype(f32)

    send0[0] = jit
    send0[1] = x
    send0[2] = pol0 + flag_tile(FLAG_TILES)
    for n in range(FLAG_TILES):
        sendf[n] = flag_tile(n)
    own = 4
    recv0[own] = send0[...]
    recvf[own] = sendf[...]

    real = pl.ds(0, EDGE)

    def halo_start(index, src, get_dst, wanted=lambda o: True):
        for oy in (-1, 1, 0):
            for oz in (-1, 1, 0):
                for ox in (1, 0):
                    if (ox, oy, oz) == (0, 0, 0) or not wanted((ox, oy, oz)):
                        continue
                    back = ox * 9 + (1 - oy) * 3 + 1 - oz
                    pltpu.make_async_remote_copy(
                        src_ref=src, dst_ref=get_dst(back),
                        send_sem=halo_send.at[index], recv_sem=halo_recv.at[index],
                        device_id=at(ox, oy, oz), device_id_type=MESH,
                    ).start()

    def halo_all(index):
        some = pl.ds(0, 17)
        ref = {
            0: recv0.at[some, :, real],
            3: recvf.at[pl.ds(0, 9), :, real], 4: recvf.at[pl.ds(0, 8), :, real],
            1: recv1.at[0, some, real], 2: recv1.at[1, some, real],
        }[index]
        return pltpu.make_async_remote_copy(
            src_ref=ref, dst_ref=ref, send_sem=halo_send.at[index], recv_sem=halo_recv.at[index],
            device_id=at(1, 0, 0), device_id_type=MESH,
        )

    def assemble(get, c, target, fill=0.0):
        full = []
        for h in range(2):
            part = []
            for b in range(3):
                m = [roll(get(h * 9 + b * 3 + k), 108 * b + EDGE * (k - c)) for k in range(3)]
                part.append(jnp.where(zone[b][0], m[0], jnp.where(zone[b][1], m[1], m[2])))
            full.append((
                jnp.where(lane < 108, part[0], part[1]),
                jnp.where(lane < 88, part[1], part[2]),
                jnp.where(lane < 68, part[2], fill),
            ))
        for t in range(3):
            target[t, 2:8, :] = full[0][t][:6]
            target[t, 8:14, :] = full[1][t][:6]
            target[t, 0:2, :] = full[1][t][4:6]
            target[t, 14:16, :] = full[0][t][:2]

    def shifted(v, i):
        dy, dz = SHIFTS[i]
        s = dy * WIDE + dz + (ORIGIN if len(v) == 3 else 0)
        if s == 0:
            return v
        r = [roll(u, -s) for u in v]
        if len(v) == 3:
            return [jnp.where(lane < LANES - s, r[t], r[t + 1]) for t in range(2)]
        if s > 0:
            return [jnp.where(lane < LANES - s, r[0], r[1]), r[1]]
        return [r[0], jnp.where(lane >= -s, r[1], r[0])]

    halves = (pl.ds(0, 8), pl.ds(8, 8))

    def in_order(shift, compute, ahead=4):
        order = [HOME] + [i for i in range(len(SHIFTS)) if i != HOME]
        for place in range(len(order) + ahead):
            if place < len(order):
                shift(order[place])
            if place >= ahead:
                compute(order[place - ahead])

    def apply(source, target, last, masked=False):
        tiles = range(3) if source is None else range(2)
        needed = [
            {FLAGS[tuple(-v for v in (dx, *s))][0] for dx in span if (dx, *s) < (0, 0, 0)} for s, span in zip(SHIFTS, SPAN)
        ]
        needed[HOME] = {0, 1, 2}

        def shift(i):
            for k in range(3):
                for rows in halves:
                    ref = ext.at[k] if source is None else chain.at[source, k]
                    for t, value in enumerate(shifted([ref[t, rows, :] for t in tiles], i)):
                        sh[i, t, k, rows, :] = value
                    if masked and k in needed[i]:
                        for t, value in enumerate(shifted([words[k, t, rows, :] for t in tiles], i)):
                            sword[i, t, k, rows, :] = value

        def present(i, dx, t, rt):
            d = (dx, *SHIFTS[i])
            if d > (0, 0, 0):
                c, m = FLAGS[d]
                word = sword[HOME, t, c, pl.ds(2 + 4 * rt, 8), :]
            else:
                c, m = FLAGS[tuple(-v for v in d)]
                word = sword[i, t, c, pl.ds(2 + 4 * rt + dx, 8), :]
            return (word & (1 << m)) != 0

        sides = [(t, rt) for t in range(2) for rt in range(1 if last else 2)]
        acc = {side: [None] * 3 for side in sides}

        def compute(i):
            for j, dx in enumerate(SPAN[i]):
                n = FIRST[i] + j
                for t, rt in sides:
                    v = [sh[i, t, k, pl.ds(dx + 2 + 4 * rt, 8), :] for k in range(3)]
                    u = [coef[t, rt, n, k] for k in range(3)]
                    iso = coef[t, rt, n, 3]
                    if masked:
                        there = present(i, dx, t, rt)
                        u = [jnp.where(there, value, 0.0) for value in u]
                        iso = jnp.where(there, iso, 0.0)
                        for k, value in enumerate((*u, iso)):
                            coef[t, rt, n, k] = value
                    dot = u[0] * v[0] + u[1] * v[1] + u[2] * v[2]
                    for k in range(3):
                        term = u[k] * dot - iso * v[k]
                        old = acc[t, rt][k]
                        acc[t, rt][k] = term if old is None else old + term

        in_order(shift, compute)
        for t, rt in sides:
            scale = polo[t, pl.ds(2 + 4 * rt, 8), :]
            for k in range(3):
                out = acc[t, rt][k] * scale
                chain[target, k, t, pl.ds(2 + 4 * rt, 8), :] = out
                if not last:
                    if rt == 0:
                        chain[target, k, t, 14:16, :] = out[0:2]
                    else:
                        chain[target, k, t, 0:2, :] = out[6:8]

    def pack(index):
        parts = []
        for k in range(3):
            a = OWN - EDGE * k
            r = [roll(chain[index, k, t, 2:10, :], -a) for t in range(2)]
            parts.append(jnp.where(lane < LANES - a, r[0], r[1]))
        out = jnp.where(zone[0][0], parts[0], jnp.where(zone[0][1], parts[1], parts[2]))
        return jnp.where(packed, out, 0.0)

    pl.semaphore_wait(barrier, len(greeted))
    halo_start(0, send0.at[:, real], lambda b: recv0.at[b, :, real])
    halo_start(3, sendf.at[:, real], lambda b: recvf.at[b, :, real], lambda o: o[0] == 0 or o == (1, 0, 0))
    chain[...] = jnp.zeros_like(chain)
    halo_all(0).wait_recv()

    for k in range(3):
        assemble(lambda b: recv0[b, 0], k, geo.at[k])
        assemble(lambda b: recv0[b, 1], k, ext.at[k])
    assemble(lambda b: recv0[b, 2], 0, geo.at[4], 1.0)
    geo[3] = lax.rsqrt(geo[4])
    for half in range(2):
        rows = pl.ds(8 * half, 8)
        r = [roll(geo[4, t, rows, :], -ORIGIN) for t in range(3)]
        for t in range(2):
            polo[t, rows, :] = jnp.where(lane < LANES - ORIGIN, r[t], r[t + 1])

    def geometry(t, carry):
        def shift(i):
            a = ORIGIN + SHIFTS[i][0] * WIDE + SHIFTS[i][1]
            for rows in halves:
                for k in range(4):
                    pair = [roll(geo[k, t + u, rows, :], -a) for u in range(2)]
                    sgeo[i, t, k, rows, :] = jnp.where(lane < LANES - a, pair[0], pair[1])

        def compute(i):
            for rt in range(2):
                base = 2 + 4 * rt
                for j, dx in enumerate(SPAN[i]):
                    n = FIRST[i] + j
                    d = (dx, *SHIFTS[i])
                    rows = pl.ds(base + dx, 8)
                    sep = [sgeo[i, t, k, rows, :] - sgeo[HOME, t, k, pl.ds(base, 8), :] for k in range(3)]
                    sep = [v + e * site_spacing if e else v for v, e in zip(sep, d)]
                    sq = sep[0] * sep[0] + sep[1] * sep[1] + sep[2] * sep[2]
                    inv = lax.rsqrt(sq)
                    roots = sgeo[HOME, t, 3, pl.ds(base, 8), :] * sgeo[i, t, 3, rows, :]
                    damp = (thole_damping * roots) * (sq * (sq * inv))
                    fall = jnp.exp(-damp)
                    inv2 = inv * inv
                    inv3 = inv2 * inv
                    rad = (1.0 - (1.0 + damp) * fall) * (3.0 * inv3 * inv2)
                    root = rad * lax.rsqrt(rad)
                    for k in range(3):
                        coef[t, rt, n, k] = root * sep[k]
                    coef[t, rt, n, 3] = (1.0 - fall) * inv3

        in_order(shift, compute)
        return carry

    lax.fori_loop(0, 2, geometry, 0)

    halo_all(3).wait_recv()
    for b in range(9):
        if b != own:
            pltpu.make_async_remote_copy(
                src_ref=recvf.at[b, :, real], dst_ref=recvf.at[9 + b, :, real],
                send_sem=halo_send.at[4], recv_sem=halo_recv.at[4],
                device_id=at(1, 0, 0), device_id_type=MESH,
            ).start()
    flagged = []
    for b in range(18):
        if b == 9:
            halo_all(4).wait_recv()
        total = jnp.where(zone[0][0], 0.0, recv0[b, 2]) * float(2 ** FLAG_TILES)
        for n in range(FLAG_TILES):
            total = total + recvf[b, n] * float(2 ** n)
        flagged.append(total.astype(jnp.int32))
    for k in range(3):
        assemble(lambda b: flagged[b], k, words.at[k], 0)

    def dots_start(index, vectors, number):
        line = jnp.zeros((1, LANES), f32)
        for m in range(number):
            value = weight * vectors[m // 2] * vectors[(m + 1) // 2]
            value = jnp.sum(jnp.sum(value, axis=0, keepdims=True), axis=1, keepdims=True)
            line = jnp.where(pick == m, value, line)
        dot_src[index] = line
        dot_dst[index, rank] = line
        for o in others:
            pltpu.make_async_remote_copy(
                src_ref=dot_src.at[index], dst_ref=dot_dst.at[index, rank],
                send_sem=dot_send.at[index], recv_sem=dot_recv.at[index],
                device_id=at(*o), device_id_type=MESH,
            ).start()

    def dots_all(index):
        some = dot_dst.at[index, pl.ds(0, count - 1)]
        return pltpu.make_async_remote_copy(
            src_ref=some, dst_ref=some, send_sem=dot_send.at[index], recv_sem=dot_recv.at[index],
            device_id=at(1, 0, 0), device_id_type=MESH,
        )

    def dots_finish(index, number):
        dots_all(index).wait_recv()
        line = jnp.sum(dot_dst[index, :, 0, :], axis=0, keepdims=True)
        return [
            jnp.broadcast_to(jnp.sum(jnp.where(pick == m, line, 0.0), axis=1, keepdims=True), (ROWS, LANES))
            for m in range(number)
        ]

    def scalars(moments, history, steps):
        number = 2 * steps
        before = [0.0] * number
        if history:
            _, _, mu1, eta1, inv1, _ = history[-1]
            _, _, mu2, eta2, inv2, _ = history[-2]
            before[1] = moments[0] * inv1
            before[2] = moments[1] * inv1 + mu1 * before[1]
            older2 = before[1] * inv2
            before[3] = moments[2] * inv1 + mu1 * before[2] + eta1 * older2
            older3 = before[2] * inv2 + mu2 * older2
            before[4] = moments[3] * inv1 + mu1 * before[3] + eta1 * older3
        now, lead, seen = list(moments), None, 0.0
        out = []
        known = list(history)
        for i in range(steps):
            gamma = now[i] if lead is None else lead * now[i]
            if known:
                eta = gamma * known[-1][4] / known[-1][5]
                beta = eta * known[-1][0]
            else:
                eta = beta = jnp.zeros((ROWS, LANES), f32)
            ratio = now[i + 1] / now[i]
            mu = ratio - seen
            seen = ratio
            inv = 1.0 - mu - eta
            alpha = 1.0 / inv
            later = [0.0] * number
            for m in range(i + 1, number - 1 - i):
                later[m] = alpha * (now[m + 1] - mu * now[m] - eta * before[m])
            before, now = now, later
            lead = alpha if lead is None else lead * alpha
            out.append((alpha, beta, mu, eta, inv, gamma))
            known.append(out[-1])
        return out

    known = []
    table = [[]]

    def lanczos(vectors):
        i = len(table) - 1
        alpha, _, mu, eta, _, _ = known[i]
        now = table[i]
        table.append([
            alpha * (now[m + 1] - mu * now[m] - (eta * table[i - 1][m] if i else 0.0))
            for m in range(vectors)
        ])

    def chain_of_three(powers, first=False, between=None):
        for k in range(3):
            if k == 2 and between is not None:
                between()
            apply(None if k == 0 else k - 1, k, k == 2, first and k == 0)
            powers.append(pack(k))

    def share(index, value):
        send1[index] = value
        recv1[index, own] = value
        halo_start(1 + index, send1.at[index, real], lambda b: recv1.at[index, b, real])

    def receive(index):
        halo_all(1 + index).wait_recv()
        for k in range(3):
            assemble(lambda b: recv1[index, b], k, ext.at[k])

    def after_first():
        known.extend(scalars(dots_finish(0, 4), known, 2))

    def after_second():
        known.extend(scalars(dots_finish(1, 6), known, 3))

    chain_of_three(table[0], first=True)
    share(0, table[0][2])
    dots_start(0, table[0], 4)
    receive(0)
    chain_of_three(table[0], between=after_first)
    lanczos(5)
    lanczos(4)
    share(1, table[2][3])
    dots_start(1, table[2], 6)
    receive(1)
    chain_of_three(table[2], between=after_second)
    table[1].append(table[2][4] * known[1][4] + known[1][2] * table[1][4] + known[1][3] * table[0][4])
    for vectors in (6, 5, 4):
        lanczos(vectors)
    dots_start(2, table[5], 6)
    known += scalars(dots_finish(2, 6), known, 3)
    for vectors in (3, 2, 1):
        lanczos(vectors)

    line = jnp.zeros((1, LANES), f32)
    p = None
    for i, (alpha, beta, *_) in enumerate(known):
        p = table[i][0] if p is None else table[i][0] + beta * p
        x = x + alpha * p
        line = jnp.where(pick == i, alpha[0:1], line)
    residual = table[ITERS][0] * weight
    out_ref[0] = x
    out_ref[1] = residual
    out_ref[2, 0:1, :] = line

    for index in range(5):
        halo_all(index).wait_send()
    for index in range(3):
        dots_all(index).wait_send()


def unpack(in_ref, x_out, r_out, len_out):
    for k, ref in enumerate((x_out, r_out)):
        value = in_ref[k]
        for y in range(EDGE):
            for c in range(3):
                ref[:, y, c, :] = roll(value, -(y * WIDE + c * EDGE))[:EDGE, :EDGE]
    len_out[...] = in_ref[2, 0:1, :ITERS]


def solution(mesh):
    sizes = tuple(mesh.shape[a] for a in ("gx", "gy", "gz"))
    assert sizes[0] == 2
    count = sizes[0] * sizes[1] * sizes[2]

    def local(permanent_field, polar, jitter, neighbors):
        assert polar.shape == (EDGE, EDGE, EDGE)
        vmem = pl.BlockSpec(memory_space=pltpu.VMEM)
        shape = jax.ShapeDtypeStruct((EDGE, EDGE, 3, EDGE), f32)
        wide, near = (3, 16, LANES), (2, 16, LANES)
        shifts = len(SHIFTS)
        anywhere = pl.BlockSpec(memory_space=pl.ANY)
        packed = pl.pallas_call(
            functools.partial(kernel, sizes),
            out_shape=pltpu.VMEM((3, ROWS, LANES), f32),
            in_specs=[anywhere] * 4,
            out_specs=vmem,
            scratch_shapes=[
                pltpu.VMEM((EDGE, EDGE, 3, EDGE), f32),
                pltpu.VMEM((EDGE, EDGE, EDGE), f32),
                pltpu.VMEM((EDGE, EDGE, 3, EDGE), f32),
                pltpu.VMEM(neighbors.shape, jnp.int32),
                pltpu.VMEM((3, *wide), f32),
                pltpu.VMEM((shifts, 2, 3, 16, LANES), f32),
                pltpu.VMEM((5, *wide), f32),
                pltpu.VMEM((3, *wide), jnp.int32),
                pltpu.VMEM((shifts, 2, 4, 16, LANES), f32),
                pltpu.VMEM((shifts, 2, 3, 16, LANES), jnp.int32),
                pltpu.VMEM(near, f32),
                pltpu.VMEM((2, 2, len(STENCIL), 4, ROWS, LANES), f32),
                pltpu.VMEM((3, 3, *near), f32),
                pltpu.VMEM((TILES, ROWS, LANES), f32),
                pltpu.VMEM((18, TILES, ROWS, LANES), f32),
                pltpu.VMEM((FLAG_TILES, ROWS, LANES), f32),
                pltpu.VMEM((18, FLAG_TILES, ROWS, LANES), f32),
                pltpu.VMEM((2, ROWS, LANES), f32),
                pltpu.VMEM((2, 18, ROWS, LANES), f32),
                pltpu.VMEM((3, 1, LANES), f32),
                pltpu.VMEM((3, count, 1, LANES), f32),
                pltpu.SemaphoreType.DMA((5,)),
                pltpu.SemaphoreType.DMA((5,)),
                pltpu.SemaphoreType.DMA((3,)),
                pltpu.SemaphoreType.DMA((3,)),
                pltpu.SemaphoreType.DMA((4,)),
            ],
            compiler_params=pltpu.CompilerParams(collective_id=0, has_side_effects=True),
        )(
            jnp.moveaxis(permanent_field, -1, 2),
            polar,
            jnp.moveaxis(jitter, -1, 2),
            neighbors,
        )
        x, r, steps = pl.pallas_call(
            unpack,
            out_shape=(shape, shape, jax.ShapeDtypeStruct((1, ITERS), f32)),
            in_specs=[vmem],
            out_specs=(vmem, vmem, vmem),
        )(pltpu.with_memory_space_constraint(packed, pltpu.VMEM))
        return jnp.moveaxis(x, 2, -1), jnp.moveaxis(r, 2, -1), steps.reshape(ITERS)

    return jax.shard_map(
        local,
        mesh=mesh,
        in_specs=(
            P("gx", "gy", "gz", None),
            P("gx", "gy", "gz"),
            P("gx", "gy", "gz", None),
            P("gx", "gy", "gz", None),
        ),
        out_specs=(P("gx", "gy", "gz", None), P("gx", "gy", "gz", None), P()),
        check_vma=False,
    )
```
